256 devices in a mesh: gz: 64 (over y, z, core), rows: 4 (over x).
Axes of the slice: x: 4, y: 4, z: 8, core: 2. Of those that a mesh axis runs over, the one named last changes fastest.
Arguments:
- forces: float32 [2, 6144, 4096], P(None, 'gz', 'rows'), may hold values from -40 to 40
- start: float32 [2, 6144, 4096], P(None, 'gz', 'rows'), may hold values from -4 to 4
- spring_bits: int32 [6144, 4096], P('gz', 'rows'), may hold values from 0 to 63, as said below
- plane_stiffness: float32 [6144], P('gz'), may hold values from 0.5 to 2
- cross_weight: float32 [3, 6144], P(None, 'gz'), may hold values from 0.1 to 1
- anchors: int32 [64], replicated, may hold values from 0 to 6143
Outputs:
- solution: float32 [2, 6144, 4096], P(None, 'gz', 'rows')
- residual: float32 [2, 6144, 4096], P(None, 'gz', 'rows')
The draws below stay inside these ranges and needn't reach their ends.
Inputs may be any that keep to these rules, and one draw needn't show every extreme that they name: `spring_bits`: bit 0: right edge present; bit 1: down edge; bit 2: diagonal edge; bit 2 + j: spring to the section j before, for j = 1 to 3. `anchors`: repeats possible.
All inputs are finite; a program needn't handle non-finite values.
Results may differ from the reference program's by a relative error of at most 0.00023.
Values sent between devices are 32-bit elements; how exact they have to be, the bound alone decides.
A program may use at most 64 MiB of HBM per device.

```python
import math
import jax
import jax.numpy as jnp

GRID = 64
PRED = 3
ITERS = 2
NSEC = 6144
NODES = 4096
ANCHORS = 64


def draw_forces(key, part):
    subkeys = jax.random.split(jax.random.fold_in(key, 11), 3)
    position = jnp.arange(NSEC, dtype=jnp.float32) / (NSEC - 1)
    section_scale = 3.0 ** position * 10.0 ** jax.random.uniform(subkeys[0], (NSEC,), jnp.float32)
    node_scale = 10.0 ** (0.5 * jax.random.uniform(subkeys[1], (NODES,), jnp.float32))
    jitter = jax.random.truncated_normal(subkeys[2], -4.0, 4.0, (2, NSEC, NODES), jnp.float32)
    return (0.1 * jitter * section_scale[None, :, None] * node_scale[None, None, :]).astype(jnp.float32)


def draw_spring_bits(key, part):
    packed = jnp.zeros((NSEC, NODES), jnp.int32)
    for bit_index in range(3 + PRED):
        rolled = jax.random.randint(jax.random.fold_in(key, 100 + bit_index), (NSEC, NODES), 0, 100)
        packed = packed + (rolled < 85).astype(jnp.int32) * 2 ** bit_index
    return packed


def place_ends(result, key, low, high):
    shape = result.shape
    index_at = [jax.random.randint(jax.random.fold_in(key, axis), (), 0, shape[axis]) for axis in range(len(shape))]
    result = result.at[tuple(index_at)].set(low)
    longest = shape.index(max(shape))
    index_at[longest] = (index_at[longest] + 1) % shape[longest]
    return result.at[tuple(index_at)].set(high)


def steps_of(key, dims, cuts, least, top_value):
    gain, own = 1.0, jax.random.fold_in(key, 6)
    for dim, shards_of in cuts:
        steps = jnp.exp(jax.random.uniform(jax.random.fold_in(own, dim), (shards_of,), jnp.float32, least / len(cuts), top_value / len(cuts)))
        gain = gain * jnp.repeat(steps, dims[dim] // shards_of).reshape([-1 if axis == dim else 1 for axis in range(len(dims))])
    return gain


def scatter_about(rng, extent, deviation, reach, cuts=(), kind=jnp.bfloat16):
    values = jax.random.normal(rng, extent, jnp.float32) * deviation
    if len(cuts) > 0:
        values = steps_of(rng, extent, cuts, -0.22, 0.18) * values
    return jnp.clip(values, min=-reach, max=reach).astype(kind)


def setup_inputs(seed: int = 0) -> dict:
    seeds = jax.random.split(jax.random.key(seed), 7)
    return {
        "forces": draw_forces(jax.random.fold_in(seeds[6], 71), 0),
        "start": scatter_about(seeds[1], (2, NSEC, NODES), 0.3, 4.0, ((1, 64), (2, 4)), jnp.float32),
        "spring_bits": draw_spring_bits(jax.random.fold_in(seeds[6], 71), 0),
        "plane_stiffness": jnp.clip(jnp.exp(math.log(2.0) - 1.3862944 * jax.random.uniform(seeds[3], (NSEC,), jnp.float32) ** steps_of(seeds[3], (NSEC,), ((0, 64),), -0.2, 0.2)), 0.5, 2.0),
        "cross_weight": jnp.clip(jnp.exp(math.log(1.0) - 2.3025851 * jax.random.uniform(seeds[4], (PRED, NSEC), jnp.float32) ** steps_of(seeds[4], (PRED, NSEC), ((1, 64),), -0.2, 0.2)), 0.1, 1.0),
        "anchors": place_ends(jax.random.randint(seeds[5], (ANCHORS,), 0, NSEC), jax.random.fold_in(seeds[5], 1), 0, NSEC - 1).astype(jnp.int32),
    }


damping = 0.05
anchor_stiffness = 20.0
transverse = 0.25


def bit_plane(spring_bits, bit_index):
    return ((spring_bits // (2 ** bit_index)) % 2).astype(jnp.float32)


def edge_pull(edge_kind, weight, stretch):
    first_part = stretch[0]
    second_part = stretch[1]
    if edge_kind == "right":
        return jnp.stack([weight * first_part, weight * transverse * second_part])
    if edge_kind == "down":
        return jnp.stack([weight * transverse * first_part, weight * second_part])
    halved = 0.5 * weight
    return jnp.stack([halved * ((1.0 + transverse) * first_part + (1.0 - transverse) * second_part),
                      halved * ((1.0 - transverse) * first_part + (1.0 + transverse) * second_part)])


def springs(spring_bits, plane_stiffness, cross_weight):
    node_index = jnp.arange(NODES, dtype=jnp.int32)
    column = (node_index % GRID)[None, :]
    grid_row = (node_index // GRID)[None, :]
    section_index = jnp.arange(NSEC, dtype=jnp.int32)[:, None]
    stiffness = plane_stiffness[:, None]
    open_column = (column < GRID - 1).astype(jnp.float32)
    open_row = (grid_row < GRID - 1).astype(jnp.float32)
    w_right = stiffness * bit_plane(spring_bits, 0) * open_column
    w_down = stiffness * bit_plane(spring_bits, 1) * open_row
    w_diag = stiffness * bit_plane(spring_bits, 2) * open_column * open_row
    w_cross = [cross_weight[lag_index][:, None] * bit_plane(spring_bits, 3 + lag_index)
               * (section_index > lag_index).astype(jnp.float32) for lag_index in range(PRED)]
    return w_right, w_down, w_diag, w_cross


def operate(vector, tethers, w_right, w_down, w_diag, w_cross):
    balance = tethers[None] * vector
    for lag_index in range(PRED):
        offset = lag_index + 1
        partner = jnp.pad(vector[:, :NSEC - offset], ((0, 0), (offset, 0), (0, 0)))
        tension = w_cross[lag_index][None] * (vector - partner)
        balance = balance + tension - jnp.pad(tension[:, offset:], ((0, 0), (0, offset), (0, 0)))
    beside = jnp.pad(vector[:, :, 1:], ((0, 0), (0, 0), (0, 1)))
    tension = edge_pull("right", w_right, vector - beside)
    balance = balance + tension - jnp.pad(tension[:, :, :-1], ((0, 0), (0, 0), (1, 0)))
    beneath = jnp.pad(vector[:, :, GRID:], ((0, 0), (0, 0), (0, GRID)))
    tension = edge_pull("down", w_down, vector - beneath)
    balance = balance + tension - jnp.pad(tension[:, :, :-GRID], ((0, 0), (0, 0), (GRID, 0)))
    corners = jnp.pad(vector[:, :, GRID + 1:], ((0, 0), (0, 0), (0, GRID + 1)))
    tension = edge_pull("diag", w_diag, vector - corners)
    balance = balance + tension - jnp.pad(tension[:, :, :-(GRID + 1)], ((0, 0), (0, 0), (GRID + 1, 0)))
    return balance


def reference(forces, start, spring_bits, plane_stiffness, cross_weight, anchors):
    w_right, w_down, w_diag, w_cross = springs(spring_bits, plane_stiffness, cross_weight)
    section_index = jnp.arange(NSEC, dtype=jnp.int32)
    anchored = jnp.any(anchors[None, :] == section_index[:, None], axis=1).astype(jnp.float32)
    tethers = (damping + anchor_stiffness * anchored)[:, None]
    right_in = jnp.pad(w_right[:, :-1], ((0, 0), (1, 0)))
    down_in = jnp.pad(w_down[:, :-GRID], ((0, 0), (GRID, 0)))
    diag_in = jnp.pad(w_diag[:, :-(GRID + 1)], ((0, 0), (GRID + 1, 0)))
    cross_sum = jnp.zeros_like(w_right)
    for lag_index in range(PRED):
        offset = lag_index + 1
        cross_sum = cross_sum + w_cross[lag_index] + jnp.pad(w_cross[lag_index][offset:], ((0, offset), (0, 0)))
    shared = tethers + 0.5 * (1.0 + transverse) * (w_diag + diag_in) + cross_sum
    diag_first = shared + (w_right + right_in) + transverse * (w_down + down_in)
    diag_second = shared + transverse * (w_right + right_in) + (w_down + down_in)
    inverse = 1.0 / jnp.stack([diag_first, diag_second])

    def apply_operator(vector):
        return operate(vector, tethers, w_right, w_down, w_diag, w_cross)

    solution = start
    residual = forces - apply_operator(solution)
    precond = residual * inverse
    direction = precond
    inner_now = jnp.sum(residual * precond)
    for iteration in range(ITERS):
        mapped = apply_operator(direction)
        step_size = inner_now / jnp.sum(direction * mapped)
        solution = solution + step_size * direction
        residual = residual - step_size * mapped
        if iteration + 1 < ITERS:
            precond = residual * inverse
            inner_next = jnp.sum(residual * precond)
            direction = precond + (inner_next / inner_now) * direction
            inner_now = inner_next
    return solution, forces - apply_operator(solution)
```

```python
import functools

import jax
import jax.numpy as jnp
from jax import lax
from jax.experimental import pallas as pl
from jax.experimental.pallas import tpu as pltpu
from jax.sharding import PartitionSpec as P

GRID = 64
PRED = 3
LANES = 128
MESH = pl.DeviceIdType.MESH

damping = 0.05
anchor_stiffness = 20.0


def digit_sizes(size):
    return (4, 8, 2) if size == 64 else (1, size // 2, 2)


def stage_groups(size, rows):
    ny, nz, nc = digit_sizes(size)
    near = [(0, 0, c, x) for c in range(nc) for x in range(rows)][1:]
    far = [(y, z, 0, 0) for y in range(ny) for z in range(nz)][1:]
    return [group for group in (near, far) if group]


def kernel(
    n_gz, n_rows, n_anchors, stages,
    f_hbm, x_hbm, b_hbm, stiff_hbm, cross_hbm, anchors_hbm,
    out_x, out_r,
    stiff, cross, anchors,
    XS, FS, BS, X, Z, U, Y, W, V, R, DG, INV, WR, WD, WG, C, K, TE, KS,
    PS, HT, HB, BO, BT, PW, PI, *rest,
):
    n_stages = len(stages)
    totals_out, totals_in = rest[:n_stages], rest[n_stages : 2 * n_stages]
    load_sem, send_sem, recv_sem, tsend_sem, trecv_sem = rest[2 * n_stages :]
    sections = TE.shape[0]
    groups = sections // 8
    g, r = lax.axis_index("gz"), lax.axis_index("rows")
    has_prev, has_next, has_above, has_below = g > 0, g < n_gz - 1, r > 0, r < n_rows - 1
    prev, nxt = {"gz": g - 1, "rows": r}, {"gz": g + 1, "rows": r}
    above, below = {"gz": g, "rows": r - 1}, {"gz": g, "rows": r + 1}

    loads = [
        pltpu.make_async_copy(src, dst, load_sem.at[i])
        for i, (src, dst) in enumerate(
            [(stiff_hbm, stiff), (cross_hbm, cross), (anchors_hbm, anchors), (b_hbm, BS), (x_hbm, XS), (f_hbm, FS)]
        )
    ]
    for load in loads:
        load.start()

    ny, nz, nc = digit_sizes(n_gz)
    my_digits = (g // (nz * nc), (g // nc) % nz, g % nc, r)

    def member(offset):
        y, z, c, x = [(d + o) % n for d, o, n in zip(my_digits, offset, (ny, nz, nc, n_rows))]
        return {"gz": (y * nz + z) * nc + c, "rows": x}

    barrier = pltpu.get_barrier_semaphore()
    for here, device in ((has_prev, prev), (has_next, nxt), (has_above, above), (has_below, below)):

        @pl.when(here)
        def _():
            pl.semaphore_signal(barrier, inc=1, device_id=device, device_id_type=MESH)

    for group in stages:
        for offset in group:
            pl.semaphore_signal(barrier, inc=1, device_id=member(offset), device_id_type=MESH)

    lane = lax.broadcasted_iota(jnp.int32, (8, LANES), 1)
    sub = lax.broadcasted_iota(jnp.int32, (8, LANES), 0)
    lo = lane < GRID
    column = lane % GRID
    open_column = column < GRID - 1
    inner_row = (2 * sub + lane // GRID) < 15
    mask_right = jnp.where(open_column, 1, 0)
    mask_down = jnp.where(inner_row, 2, 0)
    mask_diag = jnp.where(open_column & inner_row, 4, 0)
    down_scale = jnp.where(lo, 0.25, 1.0).astype(jnp.float32)
    zero = jnp.zeros((8, LANES), jnp.float32)

    def half(v):
        return pltpu.roll(v, GRID, 1)

    def left(v):
        return pltpu.roll(v, LANES - 1, 1)

    def right(v):
        return pltpu.roll(v, 1, 1)

    def from_up(v):
        turned = half(v)
        return jnp.where(lo, pltpu.roll(turned, 1, 0), turned)

    def from_down(v):
        turned = half(v)
        return jnp.where(lo, turned, pltpu.roll(turned, 7, 0))

    def tile(s):
        return pl.ds(pl.multiple_of(8 * s, 8), 8)

    def raw(s):
        return pl.ds((s // 8) * 64 + s % 8, 8, stride=8)

    def pack_last(a, b):
        return jnp.where(lo, half(a), b)

    def pack_first(a, b):
        return jnp.where(lo, a, half(b))

    def last_rows(q):
        return pl.ds(64 * q + 7, 8, stride=8)

    def first_rows(q):
        return pl.ds(64 * q, 8, stride=8)

    loads[2].wait()
    base = g * sections

    def anchor_step(i, hits):
        a = anchors[i] - base
        return tuple(jnp.where(sub + 8 * q == a, 1, hit) for q, hit in enumerate(hits))

    hits = lax.fori_loop(0, n_anchors, anchor_step, tuple(jnp.zeros((8, LANES), jnp.int32) for _ in range(groups)))
    for q in range(groups):
        TE[8 * q : 8 * q + 8, :] = jnp.where(hits[q] > 0, damping + anchor_stiffness, damping).astype(jnp.float32)

    loads[0].wait()
    loads[1].wait()
    loads[3].wait()

    def weights(s):
        bits = BS[raw(s), :]
        k = jnp.full((8, LANES), stiff[s], jnp.float32)
        KS[pl.ds(s, 1), :] = jnp.full((1, LANES), stiff[s], jnp.float32)
        WR[tile(s), :] = jnp.where((bits & mask_right) != 0, k, zero)
        WD[tile(s), :] = jnp.where((bits & mask_down) != 0, k, zero)
        WG[tile(s), :] = jnp.where((bits & mask_diag) != 0, k, zero)
        for j in range(PRED):
            kj = jnp.where(base + s > j, cross[j, s], 0.0)
            K[j, tile(s), :] = jnp.where((bits & (8 << j)) != 0, jnp.full((8, LANES), kj, jnp.float32), zero)

    for s in range(PRED):
        weights(s)

    for q in range(groups // 2):
        a = BS[64 * q + 56 : 64 * q + 64, :]
        b = BS[64 * (q + groups // 2) + 56 : 64 * (q + groups // 2) + 64, :]
        BO[8 * q : 8 * q + 8, :] = jnp.where(lo, half(a), b)

    loads[4].wait()
    for c in range(2):
        for s in list(range(PRED)) + list(range(sections - PRED, sections)):
            X[c, 8 * (s + PRED) : 8 * (s + PRED) + 8, :] = XS[c, pl.ds((s // 8) * 64 + s % 8, 8, stride=8), :]
    for q in range(groups):
        rows = slice(8 * q, 8 * q + 8)
        PS[0, 0, rows, :] = pack_first(XS[0, 64 * q : 64 * q + 8, :], XS[1, 64 * q : 64 * q + 8, :])
        PS[0, 1, rows, :] = pack_last(XS[0, 64 * q + 56 : 64 * q + 64, :], XS[1, 64 * q + 56 : 64 * q + 64, :])

    near = sum(jnp.where(here, 1, 0) for here in (has_prev, has_next, has_above, has_below))
    pl.semaphore_wait(barrier, near + sum(len(group) for group in stages))

    def remote(src, dst, at, device):
        return pltpu.make_async_remote_copy(
            src_ref=src, dst_ref=dst, send_sem=send_sem.at[at], recv_sem=recv_sem.at[at],
            device_id=device, device_id_type=MESH,
        )

    edge = 8 * PRED
    own = 8 * sections

    def row_copies(t):
        return (
            (has_below, has_above, remote(PS.at[t, 1], HT.at[t], 4 * t, below)),
            (has_above, has_below, remote(PS.at[t, 0], HB.at[t], 4 * t + 1, above)),
        )

    def section_copies(t):
        v = (X, Z, U)[t]
        return (
            (has_next, has_prev, remote(v.at[:, pl.ds(own, edge)], v.at[:, pl.ds(0, edge)], 4 * t + 2, nxt)),
            (has_prev, has_next, remote(v.at[:, pl.ds(edge, edge)], v.at[:, pl.ds(own + edge, edge)], 4 * t + 3, prev)),
        )

    bits_copy = (has_below, has_above, remote(BO, BT, 12, below))
    cross_copy = (has_prev, has_next, remote(K.at[:, pl.ds(0, edge)], K.at[:, pl.ds(own, edge)], 13, prev))

    def start(copies):
        for sends, _, copy in copies:
            pl.when(sends)(copy.start)

    def arrive(copies):
        for _, receives, copy in copies:
            pl.when(receives)(copy.wait_recv)

    def sent(copies):
        for sends, _, copy in copies:
            pl.when(sends)(copy.wait_send)

    start(row_copies(0) + (bits_copy, cross_copy) + section_copies(0))

    wide = jnp.zeros((2, edge, LANES), jnp.float32)

    @pl.when(jnp.logical_not(has_prev))
    def _():
        for v in (X, Z, U):
            v[:, 0:edge, :] = wide

    @pl.when(jnp.logical_not(has_next))
    def _():
        for v in (X, Z, U):
            v[:, own + edge : own + 2 * edge, :] = wide
        K[:, own : own + edge, :] = jnp.zeros((PRED, edge, LANES), jnp.float32)

    @pl.when(jnp.logical_not(has_above))
    def _():
        HT[...] = jnp.zeros(HT.shape, jnp.float32)
        BT[...] = jnp.zeros(BT.shape, jnp.int32)

    @pl.when(jnp.logical_not(has_below))
    def _():
        HB[...] = jnp.zeros(HB.shape, jnp.float32)

    ends = list(range(PRED)) + list(range(sections - PRED, sections))
    inner = sections - 2 * PRED
    unroll = next(n for n in (3, 2, 1) if inner % n == 0)

    def over_inner(body, carry):
        def step(i, carry):
            for n in range(unroll):
                carry = body(PRED + unroll * i + n, carry)
            return carry

        return lax.fori_loop(0, inner // unroll, step, carry)

    def fill(s, carry):
        weights(s)
        for c in range(2):
            X[c, tile(s + PRED), :] = XS[c, raw(s), :]
        return carry

    over_inner(fill, 0)
    for s in range(sections - PRED, sections):
        weights(s)

    def plane(v0, v1, wr, wd, wg):
        right0, right1 = wr * (v0 - left(v0)), (0.25 * wr) * (v1 - left(v1))
        under0, under1 = from_down(v0), from_down(v1)
        down0, down1 = (0.25 * wd) * (v0 - under0), wd * (v1 - under1)
        gap0, gap1 = v0 - left(under0), v1 - left(under1)
        near_, far_ = 0.625 * wg, 0.375 * wg
        diag0, diag1 = near_ * gap0 + far_ * gap1, far_ * gap0 + near_ * gap1
        pull0 = (right0 + down0 + diag0) - right(right0) - from_up(down0 + right(diag0))
        pull1 = (right1 + down1 + diag1) - right(right1) - from_up(down1 + right(diag1))
        return pull0, pull1

    def apply(v, out, s, first=False):
        wr, wd, wg = WR[tile(s), :], WD[tile(s), :], WG[tile(s), :]
        back = [K[j, tile(s), :] for j in range(PRED)]
        ahead = [K[j, tile(s + j + 1), :] for j in range(PRED)]
        if first:
            tether = jnp.broadcast_to(TE[pl.ds(s, 1), :], (8, LANES))
            centre = tether + ((back[0] + ahead[0]) + (back[1] + ahead[1]) + (back[2] + ahead[2]))
            C[tile(s), :] = centre
            shared = centre + 0.625 * (wg + right(from_up(wg)))
            across, along = wr + right(wr), wd + from_up(wd)
            DG[0, tile(s), :] = shared + across + 0.25 * along
            DG[1, tile(s), :] = shared + 0.25 * across + along
        else:
            centre = C[tile(s), :]
        mine = [v[c, tile(s + PRED), :] for c in range(2)]
        done = []
        for c, pull in enumerate(plane(*mine, wr, wd, wg)):
            total = pull + centre * mine[c]
            for j in range(PRED):
                total = total - (
                    back[j] * v[c, tile(s + PRED - j - 1), :] + ahead[j] * v[c, tile(s + PRED + j + 1), :]
                )
            out[c, tile(s), :] = total
            done.append(total)
        return mine[0] * done[0] + mine[1] * done[1]

    def first_apply(s, carry):
        apply(X, Y, s, first=True)
        return carry

    over_inner(first_apply, 0)

    def bottom_weights(q, carry):
        rows = tile(q)
        bits = BS[pl.ds(pl.multiple_of(64 * q + 56, 8), 8), :]
        bits = jnp.where(lo, half(bits), bits)
        k = jnp.where(has_below, KS[rows, :], zero)
        PW[2, rows, :] = jnp.where((bits & 2) != 0, k, zero) * down_scale
        PW[3, rows, :] = jnp.where(((bits & 4) != 0) & open_column, k, zero)
        return carry

    lax.fori_loop(0, groups, bottom_weights, 0)

    arrive((bits_copy,))

    def top_weights(q, carry):
        both = BT[tile(q), :]
        for n, bits in enumerate((jnp.where(lo, both, half(both)), jnp.where(lo, half(both), both))):
            rows = tile(q + n * (groups // 2))
            k = jnp.where(has_above, KS[rows, :], zero)
            PW[0, rows, :] = jnp.where((bits & 2) != 0, k, zero) * down_scale
            PW[1, rows, :] = jnp.where(((bits & 4) != 0) & open_column, k, zero)
        return carry

    lax.fori_loop(0, groups // 2, top_weights, 0)

    def outside(t, q):
        rows = tile(q)
        mine, other = PS[t, 0, rows, :], HT[t, rows, :]
        gap = other - left(mine)
        top = PW[0, rows, :] * (mine - other) - right(PW[1, rows, :] * (0.625 * gap + 0.375 * half(gap)))
        mine, other = PS[t, 1, rows, :], HB[t, rows, :]
        gap = mine - left(other)
        bottom = PW[2, rows, :] * (mine - other) + PW[3, rows, :] * (0.625 * gap + 0.375 * half(gap))
        return top, bottom

    def add_rows(ref, q, top, bottom):
        a, b = ref[0, first_rows(q), :], ref[1, first_rows(q), :]
        a, b = a + jnp.where(lo, top, zero), b + jnp.where(lo, half(top), zero)
        ref[0, first_rows(q), :] = a
        ref[1, first_rows(q), :] = b
        first = pack_first(a, b)
        a, b = ref[0, last_rows(q), :], ref[1, last_rows(q), :]
        a, b = a + jnp.where(lo, zero, half(bottom)), b + jnp.where(lo, zero, bottom)
        ref[0, last_rows(q), :] = a
        ref[1, last_rows(q), :] = b
        return first, pack_last(a, b)

    arrive((cross_copy,) + section_copies(0))
    for s in ends:
        first_apply(s, 0)
    arrive(row_copies(0))

    def edge_residual(q, carry):
        rows = tile(q)
        top, bottom = outside(0, q)
        y = add_rows(Y, q, top, bottom)
        d = add_rows(
            DG, q, PW[0, rows, :] + 0.625 * right(PW[1, rows, :]), PW[2, rows, :] + 0.625 * PW[3, rows, :]
        )
        head = pl.ds(pl.multiple_of(64 * q, 8), 8)
        foot = pl.ds(pl.multiple_of(64 * q + 56, 8), 8)
        f = (pack_first(FS[0, head, :], FS[1, head, :]), pack_last(FS[0, foot, :], FS[1, foot, :]))
        for n in range(2):
            inverse = 1.0 / d[n]
            PI[n, rows, :] = inverse
            PS[1, n, rows, :] = (f[n] - y[n]) * inverse
        return carry

    loads[5].wait()
    lax.fori_loop(0, groups, edge_residual, 0)
    start(row_copies(1))

    def residual(s, total):
        for c in range(2):
            inverse = 1.0 / DG[c, tile(s), :]
            res = FS[c, raw(s), :] - Y[c, tile(s), :]
            pre = res * inverse
            INV[c, tile(s), :] = inverse
            R[c, tile(s), :] = res
            Z[c, tile(s + PRED), :] = pre
            total = total + res * pre
        return total

    sum0 = zero
    for s in ends:
        sum0 = residual(s, sum0)
    start(section_copies(1))
    sum0 = over_inner(residual, sum0)

    def second_apply(s, carry):
        apply(Z, W, s)
        return carry

    over_inner(second_apply, 0)

    arrive(section_copies(1))
    for s in ends:
        second_apply(s, 0)
    arrive(row_copies(1))

    def edge_second(q, carry):
        rows = tile(q)
        w = add_rows(W, q, *outside(1, q))
        for n in range(2):
            PS[2, n, rows, :] = w[n] * PI[n, rows, :]
        return carry

    lax.fori_loop(0, groups, edge_second, 0)
    start(row_copies(2))

    def second(s, totals):
        sum1, sum2 = totals
        for c in range(2):
            w = W[c, tile(s), :]
            u = w * INV[c, tile(s), :]
            U[c, tile(s + PRED), :] = u
            sum1 = sum1 + w * Z[c, tile(s + PRED), :]
            sum2 = sum2 + w * u
        return sum1, sum2

    sums = (zero, zero)
    for s in ends:
        sums = second(s, sums)
    start(section_copies(2))
    sum1, sum2 = over_inner(second, sums)
    sum3 = over_inner(lambda s, total: total + apply(U, V, s), zero)

    arrive(section_copies(2))
    for s in ends:
        sum3 = sum3 + apply(U, V, s)
    arrive(row_copies(2))

    def edge_third(q, total):
        rows = tile(q)
        top, bottom = outside(2, q)
        add_rows(V, q, top, bottom)
        return total + (top * PS[2, 0, rows, :] + bottom * PS[2, 1, rows, :])

    sum3 = lax.fori_loop(0, groups, edge_third, sum3)

    row = zero
    for n, part in enumerate((sum0, sum1, sum2, sum3)):
        part = part + half(part)
        part = part + pltpu.roll(part, 32, 1)
        row = jnp.where(lane // 32 == n, part, row)
    row = jnp.sum(row, axis=0, keepdims=True)
    pending = []
    for t, group in enumerate(stages):
        totals_out[t][0] = row
        for n, offset in enumerate(group):
            copy = pltpu.make_async_remote_copy(
                src_ref=totals_out[t].at[0], dst_ref=totals_in[t].at[n],
                send_sem=tsend_sem.at[t], recv_sem=trecv_sem.at[t],
                device_id=member(offset), device_id_type=MESH,
            )
            copy.start()
        everyone = pltpu.make_async_remote_copy(
            src_ref=totals_in[t], dst_ref=totals_in[t], send_sem=tsend_sem.at[t], recv_sem=trecv_sem.at[t],
            device_id=member(group[0]), device_id_type=MESH,
        )
        everyone.wait_recv()
        pending.append(everyone)
        row = row + jnp.sum(totals_in[t][...], axis=0)

    lanes = lax.broadcasted_iota(jnp.int32, (1, LANES), 1) // 32
    c0, c1, c2, c3 = [jnp.sum(jnp.where(lanes == n, row, 0.0), axis=1, keepdims=True) for n in range(4)]
    alpha0 = c0 / c1
    inner1 = alpha0 * alpha0 * c2 - c0
    growth = 1.0 + inner1 / c0
    alpha1 = inner1 / (growth * growth * c1 - 2.0 * growth * alpha0 * c2 + alpha0 * alpha0 * c3)
    along = jnp.broadcast_to(alpha0 + alpha1 * growth, (8, LANES))
    against = jnp.broadcast_to(alpha1 * alpha0, (8, LANES))

    def finish(q, carry):
        for n in range(8):
            s = 8 * q + n
            for c in range(2):
                to = pl.ds(64 * q + n, 8, stride=8)
                z, u = Z[c, tile(s + PRED), :], U[c, tile(s + PRED), :]
                out_x[c, to, :] = X[c, tile(s + PRED), :] + (along * z - against * u)
                out_r[c, to, :] = R[c, tile(s), :] - (along * W[c, tile(s), :] - against * V[c, tile(s), :])
        return carry

    lax.fori_loop(0, groups, finish, 0)

    for t in range(3):
        sent(row_copies(t) + section_copies(t))
    sent((bits_copy, cross_copy))
    for copy in pending:
        copy.wait_send()


def tiles(shard):
    *lead, sections, nodes = shard.shape
    split = shard.reshape(*lead, sections // 8, 8, nodes // LANES, LANES)
    return jnp.swapaxes(split, -3, -2).reshape(*lead, sections * nodes // LANES, LANES)


def untiled(rows, sections, nodes):
    lead = rows.shape[:-2]
    split = rows.reshape(*lead, sections // 8, nodes // LANES, 8, LANES)
    return jnp.swapaxes(split, -3, -2).reshape(*lead, sections, nodes)


def per_device(n_gz, n_rows, forces, start, spring_bits, plane_stiffness, cross_weight, anchors):
    _, sections, nodes = forces.shape
    stages = stage_groups(n_gz, n_rows)
    f32 = functools.partial(pltpu.VMEM, dtype=jnp.float32)
    own, held = 8 * sections, 8 * (sections + 2 * PRED)
    scratch = [
        pltpu.SMEM((sections,), jnp.float32),
        pltpu.SMEM((PRED, sections), jnp.float32),
        pltpu.SMEM(anchors.shape, jnp.int32),
        f32((2, own, LANES)),
        f32((2, own, LANES)),
        pltpu.VMEM((own, LANES), jnp.int32),
        *[f32((2, held, LANES)) for _ in range(3)],
        *[f32((2, own, LANES)) for _ in range(6)],
        *[f32((own, LANES)) for _ in range(4)],
        f32((PRED, own + 8 * PRED, LANES)),
        f32((sections, LANES)),
        f32((sections, LANES)),
        f32((3, 2, sections, LANES)),
        f32((3, sections, LANES)),
        f32((3, sections, LANES)),
        pltpu.VMEM((sections // 2, LANES), jnp.int32),
        pltpu.VMEM((sections // 2, LANES), jnp.int32),
        f32((4, sections, LANES)),
        f32((2, sections, LANES)),
        *[f32((1, 1, LANES)) for _ in stages],
        *[f32((len(group), 1, LANES)) for group in stages],
        pltpu.SemaphoreType.DMA((6,)),
        pltpu.SemaphoreType.DMA((14,)),
        pltpu.SemaphoreType.DMA((14,)),
        pltpu.SemaphoreType.DMA((len(stages),)),
        pltpu.SemaphoreType.DMA((len(stages),)),
    ]
    shape = jax.ShapeDtypeStruct((2, own, LANES), jnp.float32)
    solved, left_over = pl.pallas_call(
        functools.partial(kernel, n_gz, n_rows, anchors.shape[0], stages),
        out_shape=(shape, shape),
        in_specs=[pl.BlockSpec(memory_space=pl.ANY)] * 6,
        out_specs=[pl.BlockSpec(memory_space=pltpu.VMEM)] * 2,
        scratch_shapes=scratch,
        compiler_params=pltpu.CompilerParams(
            collective_id=0, has_side_effects=True, vmem_limit_bytes=40 * 1024 * 1024
        ),
        name="cg",
    )(tiles(forces), tiles(start), tiles(spring_bits), plane_stiffness, cross_weight, anchors)
    return untiled(solved, sections, nodes), untiled(left_over, sections, nodes)


def solution(mesh):
    return jax.shard_map(
        functools.partial(per_device, mesh.shape["gz"], mesh.shape["rows"]),
        mesh=mesh,
        in_specs=(P(None, "gz", "rows"), P(None, "gz", "rows"), P("gz", "rows"), P("gz"), P(None, "gz"), P()),
        out_specs=(P(None, "gz", "rows"), P(None, "gz", "rows")),
        check_vma=False,
    )
```

```python
import functools

import jax
import jax.numpy as jnp
from jax import lax
from jax.experimental import pallas as pl
from jax.experimental.pallas import tpu as pltpu
from jax.sharding import PartitionSpec as P

GRID = 64
PRED = 3
LANES = 128
APPLY_UNROLL = 10
MESH = pl.DeviceIdType.MESH

damping = 0.05
anchor_stiffness = 20.0


def digit_sizes(size):
    return (4, 8, 2) if size == 64 else (1, size // 2, 2)


def stage_groups(size, rows):
    ny, nz, nc = digit_sizes(size)
    near = [(0, 0, c, x) for c in range(nc) for x in range(rows)][1:]
    far = [(y, z, 0, 0) for y in range(ny) for z in range(nz)][1:]
    return [group for group in (near, far) if group]


def kernel(
    n_gz, n_rows, n_anchors, stages,
    f_hbm, x_hbm, b_hbm, stiff_hbm, cross_hbm, anchors_hbm,
    out_x, out_r,
    stiff, cross, anchors,
    XS, FS, BS, X, Z, U, Y, W, V, R, INV, DG, WP, K, TE, KS,
    PS, HT, HB, BO, BT, PW, PI, PY, PH, PF, FX, *rest,
):
    n_stages = len(stages)
    totals_out, totals_in = rest[:n_stages], rest[n_stages : 2 * n_stages]
    load_sem, send_sem, recv_sem, tsend_sem, trecv_sem = rest[2 * n_stages :]
    sections = TE.shape[0]
    groups = sections // 8
    g, r = lax.axis_index("gz"), lax.axis_index("rows")
    has_prev, has_next, has_above, has_below = g > 0, g < n_gz - 1, r > 0, r < n_rows - 1
    prev, nxt = {"gz": g - 1, "rows": r}, {"gz": g + 1, "rows": r}
    above, below = {"gz": g, "rows": r - 1}, {"gz": g, "rows": r + 1}

    loads = [
        pltpu.make_async_copy(src, dst, load_sem.at[i])
        for i, (src, dst) in enumerate(
            [(stiff_hbm, stiff), (cross_hbm, cross), (anchors_hbm, anchors), (b_hbm, BS), (x_hbm, XS), (f_hbm, FS)]
        )
    ]
    for load in loads:
        load.start()

    ny, nz, nc = digit_sizes(n_gz)
    my_digits = (g // (nz * nc), (g // nc) % nz, g % nc, r)

    def member(offset):
        y, z, c, x = [(d + o) % n for d, o, n in zip(my_digits, offset, (ny, nz, nc, n_rows))]
        return {"gz": (y * nz + z) * nc + c, "rows": x}

    barrier = pltpu.get_barrier_semaphore()
    for here, device in ((has_prev, prev), (has_next, nxt), (has_above, above), (has_below, below)):

        @pl.when(here)
        def _():
            pl.semaphore_signal(barrier, inc=1, device_id=device, device_id_type=MESH)

    for group in stages:
        for offset in group:
            pl.semaphore_signal(barrier, inc=1, device_id=member(offset), device_id_type=MESH)

    lane = lax.broadcasted_iota(jnp.int32, (8, LANES), 1)
    sub = lax.broadcasted_iota(jnp.int32, (8, LANES), 0)
    lo = lane < GRID
    column = lane % GRID
    open_column = column < GRID - 1
    inner_row = (2 * sub + lane // GRID) < 15
    mask_right = jnp.where(open_column, 1, 0)
    mask_down = jnp.where(inner_row, 2, 0)
    mask_diag = jnp.where(open_column & inner_row, 4, 0)
    down_scale = jnp.where(lo, 0.25, 1.0).astype(jnp.float32)
    zero = jnp.zeros((8, LANES), jnp.float32)

    def half(v):
        return pltpu.roll(v, GRID, 1)

    def left(v):
        return pltpu.roll(v, LANES - 1, 1)

    def right(v):
        return pltpu.roll(v, 1, 1)

    def lowered(v, by):
        return pltpu.roll(jnp.where(lo, v, pltpu.roll(v, 1, 0)), by, 1)

    def tile(s):
        return pl.ds(pl.multiple_of(8 * s, 8), 8)

    def raw(s):
        return pl.ds((s // 8) * 64 + s % 8, 8, stride=8)

    def pack_last(a, b):
        return jnp.where(lo, half(a), b)

    def pack_first(a, b):
        return jnp.where(lo, a, half(b))

    loads[2].wait()
    base = g * sections

    def anchor_step(i, hits):
        a = anchors[i] - base
        return tuple(jnp.where(sub + 8 * q == a, 1, hit) for q, hit in enumerate(hits))

    hits = lax.fori_loop(0, n_anchors, anchor_step, tuple(jnp.zeros((8, LANES), jnp.int32) for _ in range(groups)))
    for q in range(groups):
        TE[8 * q : 8 * q + 8, :] = jnp.where(hits[q] > 0, damping + anchor_stiffness, damping).astype(jnp.float32)

    loads[0].wait()
    loads[1].wait()
    loads[3].wait()

    def cross_weights(s):
        bits = BS[raw(s), :]
        KS[pl.ds(s, 1), :] = jnp.full((1, LANES), stiff[s], jnp.float32)
        for j in range(PRED):
            kj = jnp.where(base + s > j, cross[j, s], 0.0)
            K[j, tile(s), :] = jnp.where((bits & (8 << j)) != 0, jnp.full((8, LANES), kj, jnp.float32), zero)
        return bits

    def plane_weights(s, bits):
        k = jnp.full((8, LANES), stiff[s], jnp.float32)
        wr = jnp.where((bits & mask_right) != 0, k, zero)
        wd = jnp.where((bits & mask_down) != 0, k, zero)
        wg = jnp.where((bits & mask_diag) != 0, k, zero)
        for n, w in enumerate((wr, right(wr), wd, lowered(wd, GRID), wg, lowered(wg, GRID + 1))):
            WP[n, tile(s), :] = w

    for s in range(PRED):
        cross_weights(s)

    for q in range(groups // 2):
        a = BS[64 * q + 56 : 64 * q + 64, :]
        b = BS[64 * (q + groups // 2) + 56 : 64 * (q + groups // 2) + 64, :]
        BO[8 * q : 8 * q + 8, :] = jnp.where(lo, half(a), b)

    loads[4].wait()
    for c in range(2):
        for s in list(range(PRED)) + list(range(sections - PRED, sections)):
            X[c, 8 * (s + PRED) : 8 * (s + PRED) + 8, :] = XS[c, pl.ds((s // 8) * 64 + s % 8, 8, stride=8), :]
    for q in range(groups):
        rows = slice(8 * q, 8 * q + 8)
        PS[0, 0, rows, :] = pack_first(XS[0, 64 * q : 64 * q + 8, :], XS[1, 64 * q : 64 * q + 8, :])
        PS[0, 1, rows, :] = pack_last(XS[0, 64 * q + 56 : 64 * q + 64, :], XS[1, 64 * q + 56 : 64 * q + 64, :])

    near = sum(jnp.where(here, 1, 0) for here in (has_prev, has_next, has_above, has_below))
    pl.semaphore_wait(barrier, near + sum(len(group) for group in stages))

    def remote(src, dst, at, device):
        return pltpu.make_async_remote_copy(
            src_ref=src, dst_ref=dst, send_sem=send_sem.at[at], recv_sem=recv_sem.at[at],
            device_id=device, device_id_type=MESH,
        )

    edge = 8 * PRED
    own = 8 * sections

    def row_copies(t):
        return (
            (has_below, has_above, remote(PS.at[t, 1], HT.at[t], 4 * t, below)),
            (has_above, has_below, remote(PS.at[t, 0], HB.at[t], 4 * t + 1, above)),
        )

    def section_copies(t):
        v = (X, Z, U)[t]
        return (
            (has_next, has_prev, remote(v.at[:, pl.ds(own, edge)], v.at[:, pl.ds(0, edge)], 4 * t + 2, nxt)),
            (has_prev, has_next, remote(v.at[:, pl.ds(edge, edge)], v.at[:, pl.ds(own + edge, edge)], 4 * t + 3, prev)),
        )

    bits_copy = (has_below, has_above, remote(BO, BT, 12, below))
    cross_copy = (has_prev, has_next, remote(K.at[:, pl.ds(0, edge)], K.at[:, pl.ds(own, edge)], 13, prev))

    def start(copies):
        for sends, _, copy in copies:
            pl.when(sends)(copy.start)

    def arrive(copies):
        for _, receives, copy in copies:
            pl.when(receives)(copy.wait_recv)

    def sent(copies):
        for sends, _, copy in copies:
            pl.when(sends)(copy.wait_send)

    start(row_copies(0) + (bits_copy, cross_copy) + section_copies(0))

    wide = jnp.zeros((2, edge, LANES), jnp.float32)

    @pl.when(jnp.logical_not(has_prev))
    def _():
        for v in (X, Z, U):
            v[:, 0:edge, :] = wide

    @pl.when(jnp.logical_not(has_next))
    def _():
        for v in (X, Z, U):
            v[:, own + edge : own + 2 * edge, :] = wide
        K[:, own : own + edge, :] = jnp.zeros((PRED, edge, LANES), jnp.float32)

    @pl.when(jnp.logical_not(has_above))
    def _():
        HT[...] = jnp.zeros(HT.shape, jnp.float32)
        BT[...] = jnp.zeros(BT.shape, jnp.int32)

    @pl.when(jnp.logical_not(has_below))
    def _():
        HB[...] = jnp.zeros(HB.shape, jnp.float32)

    ends = list(range(PRED)) + list(range(sections - PRED, sections))
    inner = sections - 2 * PRED

    def over_inner(body, carry, most):
        unroll = next(n for n in range(most, 0, -1) if inner % n == 0)

        def step(i, carry):
            for n in range(unroll):
                carry = body(PRED + unroll * i + n, carry)
            return carry

        return lax.fori_loop(0, inner // unroll, step, carry)

    def fill(s, carry):
        plane_weights(s, cross_weights(s))
        for c in range(2):
            X[c, tile(s + PRED), :] = XS[c, raw(s), :]
        return carry

    over_inner(fill, 0, 10)
    for s in range(PRED):
        plane_weights(s, BS[raw(s), :])
    for s in range(sections - PRED, sections):
        plane_weights(s, cross_weights(s))

    def apply(v, out, s, first=False):
        wr, wl, wd, wu, wg, wv = [WP[n, tile(s), :] for n in range(6)]
        back = [K[j, tile(s), :] for j in range(PRED)]
        ahead = [K[j, tile(s + j + 1), :] for j in range(PRED)]
        if first:
            tether = jnp.broadcast_to(TE[pl.ds(s, 1), :], (8, LANES))
            shared = tether + ((back[0] + ahead[0]) + (back[1] + ahead[1]) + (back[2] + ahead[2]))
            shared = shared + 0.625 * (wg + wv)
            across, along = wr + wl, wd + wu
            own_weight = [shared + across + 0.25 * along, shared + 0.25 * across + along]
            mixed = 0.375 * (wg + wv)
            DG[2, tile(s), :] = mixed
            for c in range(2):
                DG[c, tile(s), :] = own_weight[c]
                INV[c, tile(s), :] = 1.0 / own_weight[c]
        else:
            own_weight, mixed = [DG[c, tile(s), :] for c in range(2)], DG[2, tile(s), :]
        mine = [v[c, tile(s + PRED), :] for c in range(2)]
        sides, lines, slants = [], [], []
        for c in range(2):
            after = jnp.where(lo, v[c, pl.ds(8 * (s + PRED) + 1, 8), :], mine[c])
            before = jnp.where(lo, mine[c], v[c, pl.ds(8 * (s + PRED) - 1, 8), :])
            sides.append(wr * left(mine[c]) + wl * right(mine[c]))
            lines.append(wd * half(after) + wu * half(before))
            slants.append(wg * pltpu.roll(after, GRID - 1, 1) + wv * pltpu.roll(before, GRID + 1, 1))
        pulls = [
            (sides[0] + 0.25 * lines[0]) + (0.625 * slants[0] + 0.375 * slants[1]),
            (0.25 * sides[1] + lines[1]) + (0.375 * slants[0] + 0.625 * slants[1]),
        ]
        done = []
        for c in range(2):
            ties = [
                back[j] * v[c, tile(s + PRED - j - 1), :] + ahead[j] * v[c, tile(s + PRED + j + 1), :]
                for j in range(PRED)
            ]
            total = (own_weight[c] * mine[c] + mixed * mine[1 - c]) - (pulls[c] + (ties[0] + ties[1] + ties[2]))
            out[c, tile(s), :] = total
            done.append(total)
        return mine[0] * done[0] + mine[1] * done[1]

    def first_apply(s, carry):
        apply(X, Y, s, first=True)
        return carry

    over_inner(first_apply, 0, APPLY_UNROLL)

    def rows_of(q):
        return slice(8 * q, 8 * q + 8)

    def packed(ref, q):
        at = [[ref[c, pl.ds(64 * q + line, 8, stride=8), :] for c in range(2)] for line in (0, 7)]
        return pack_first(*at[0]), pack_last(*at[1])

    def spread(top, bottom):
        return (top, half(top)), (half(bottom), bottom)

    def change_rows(ref, q, top, bottom, change):
        for line, keep_lo, parts in zip((0, 7), (False, True), spread(top, bottom)):
            for c in range(2):
                to = pl.ds(64 * q + line, 8, stride=8)
                old = ref[c, to, :]
                new = change(old, parts[c])
                ref[c, to, :] = jnp.where(lo, old, new) if keep_lo else jnp.where(lo, new, old)

    for q in range(groups):
        rows = rows_of(q)
        bits = BS[64 * q + 56 : 64 * q + 64, :]
        bits = jnp.where(lo, half(bits), bits)
        k = jnp.where(has_below, KS[rows, :], zero)
        PW[2, rows, :] = jnp.where((bits & 2) != 0, k, zero) * down_scale
        PW[3, rows, :] = jnp.where(((bits & 4) != 0) & open_column, k, zero)

    middle = range(1, groups - 1)
    outer = sorted({0, groups - 1})

    def before_rows(t, out, some):
        for q in some:
            rows = rows_of(q)
            for n, part in enumerate(packed(out, q)):
                PY[n, rows, :] = part
                PH[n, rows, :] = half(PS[t, n, rows, :])

    def outside(t, q):
        rows = rows_of(q)
        mine, turned, other = PS[t, 0, rows, :], PH[0, rows, :], HT[t, rows, :]
        slant = 0.625 * (right(other) - mine) + 0.375 * (pltpu.roll(other, GRID + 1, 1) - turned)
        top = PW[0, rows, :] * (mine - other) - PW[1, rows, :] * slant
        mine, turned, other = PS[t, 1, rows, :], PH[1, rows, :], HB[t, rows, :]
        slant = 0.625 * (mine - left(other)) + 0.375 * (turned - pltpu.roll(other, GRID - 1, 1))
        bottom = PW[2, rows, :] * (mine - other) + PW[3, rows, :] * slant
        FX[0, rows, :] = top
        FX[1, rows, :] = bottom
        return top, bottom

    def add(old, new):
        return old + new

    def put(old, new):
        return new

    before_rows(0, Y, middle)
    loads[5].wait()
    for q in range(groups):
        rows = rows_of(q)
        head, foot = slice(64 * q, 64 * q + 8), slice(64 * q + 56, 64 * q + 64)
        PF[0, rows, :] = pack_first(FS[0, head, :], FS[1, head, :])
        PF[1, rows, :] = pack_last(FS[0, foot, :], FS[1, foot, :])

    arrive((bits_copy,))
    for q in range(groups // 2):
        both = BT[rows_of(q), :]
        for n, bits in enumerate((jnp.where(lo, both, half(both)), jnp.where(lo, half(both), both))):
            rows = rows_of(q + n * (groups // 2))
            k = jnp.where(has_above, KS[rows, :], zero)
            PW[0, rows, :] = jnp.where((bits & 2) != 0, k, zero) * down_scale
            PW[1, rows, :] = right(jnp.where(((bits & 4) != 0) & open_column, k, zero))

    arrive((cross_copy,) + section_copies(0))
    for s in ends:
        first_apply(s, 0)
    before_rows(0, Y, outer)
    for q in range(groups):
        rows = rows_of(q)
        top, bottom = packed(DG, q)
        PI[0, rows, :] = 1.0 / (top + (PW[0, rows, :] + 0.625 * PW[1, rows, :]))
        PI[1, rows, :] = 1.0 / (bottom + (PW[2, rows, :] + 0.625 * PW[3, rows, :]))
    arrive(row_copies(0))
    for q in range(groups):
        rows = rows_of(q)
        for n, part in enumerate(outside(0, q)):
            PS[1, n, rows, :] = (PF[n, rows, :] - (PY[n, rows, :] + part)) * PI[n, rows, :]
    start(row_copies(1))
    for q in range(groups):
        rows = rows_of(q)
        change_rows(Y, q, FX[0, rows, :], FX[1, rows, :], add)
        change_rows(INV, q, PI[0, rows, :], PI[1, rows, :], put)

    def residual(s, total):
        for c in range(2):
            res = FS[c, raw(s), :] - Y[c, tile(s), :]
            pre = res * INV[c, tile(s), :]
            R[c, tile(s), :] = res
            Z[c, tile(s + PRED), :] = pre
            total = total + res * pre
        return total

    sum0 = zero
    for s in ends:
        sum0 = residual(s, sum0)
    start(section_copies(1))
    sum0 = over_inner(residual, sum0, 10)

    def second_apply(s, carry):
        apply(Z, W, s)
        return carry

    over_inner(second_apply, 0, APPLY_UNROLL)
    before_rows(1, W, middle)

    arrive(section_copies(1))
    for s in ends:
        second_apply(s, 0)
    before_rows(1, W, outer)
    arrive(row_copies(1))
    for q in range(groups):
        rows = rows_of(q)
        for n, part in enumerate(outside(1, q)):
            PS[2, n, rows, :] = (PY[n, rows, :] + part) * PI[n, rows, :]
    start(row_copies(2))
    for q in range(groups):
        change_rows(W, q, FX[0, rows_of(q), :], FX[1, rows_of(q), :], add)

    def second(s, totals):
        sum1, sum2 = totals
        for c in range(2):
            w = W[c, tile(s), :]
            u = w * INV[c, tile(s), :]
            U[c, tile(s + PRED), :] = u
            sum1 = sum1 + w * Z[c, tile(s + PRED), :]
            sum2 = sum2 + w * u
        return sum1, sum2

    sums = (zero, zero)
    for s in ends:
        sums = second(s, sums)
    start(section_copies(2))
    sum1, sum2 = over_inner(second, sums, 10)
    sum3 = over_inner(lambda s, total: total + apply(U, V, s), zero, APPLY_UNROLL)
    for q in range(groups):
        for n in range(2):
            PH[n, rows_of(q), :] = half(PS[2, n, rows_of(q), :])

    arrive(section_copies(2))
    for s in ends:
        sum3 = sum3 + apply(U, V, s)
    arrive(row_copies(2))
    for q in range(groups):
        top, bottom = outside(2, q)
        sum3 = sum3 + (top * PS[2, 0, rows_of(q), :] + bottom * PS[2, 1, rows_of(q), :])

    row = zero
    for n, part in enumerate((sum0, sum1, sum2, sum3)):
        part = part + half(part)
        part = part + pltpu.roll(part, 32, 1)
        row = jnp.where(lane // 32 == n, part, row)
    row = jnp.sum(row, axis=0, keepdims=True)
    pending = []

    def finish_rows():
        for q in range(groups):
            change_rows(V, q, FX[0, rows_of(q), :], FX[1, rows_of(q), :], add)

    for t, group in enumerate(stages):
        totals_out[t][0] = row
        for n, offset in enumerate(group):
            copy = pltpu.make_async_remote_copy(
                src_ref=totals_out[t].at[0], dst_ref=totals_in[t].at[n],
                send_sem=tsend_sem.at[t], recv_sem=trecv_sem.at[t],
                device_id=member(offset), device_id_type=MESH,
            )
            copy.start()
        everyone = pltpu.make_async_remote_copy(
            src_ref=totals_in[t], dst_ref=totals_in[t], send_sem=tsend_sem.at[t], recv_sem=trecv_sem.at[t],
            device_id=member(group[0]), device_id_type=MESH,
        )
        if t == 0:
            finish_rows()
        everyone.wait_recv()
        pending.append(everyone)
        row = row + jnp.sum(totals_in[t][...], axis=0)

    lanes = lax.broadcasted_iota(jnp.int32, (1, LANES), 1) // 32
    c0, c1, c2, c3 = [jnp.sum(jnp.where(lanes == n, row, 0.0), axis=1, keepdims=True) for n in range(4)]
    alpha0 = c0 / c1
    inner1 = alpha0 * alpha0 * c2 - c0
    growth = 1.0 + inner1 / c0
    alpha1 = inner1 / (growth * growth * c1 - 2.0 * growth * alpha0 * c2 + alpha0 * alpha0 * c3)
    along = jnp.broadcast_to(alpha0 + alpha1 * growth, (8, LANES))
    against = jnp.broadcast_to(alpha1 * alpha0, (8, LANES))

    def finish(q, carry):
        for n in range(8):
            s = 8 * q + n
            for c in range(2):
                to = pl.ds(64 * q + n, 8, stride=8)
                z, u = Z[c, tile(s + PRED), :], U[c, tile(s + PRED), :]
                out_x[c, to, :] = X[c, tile(s + PRED), :] + (along * z - against * u)
                out_r[c, to, :] = R[c, tile(s), :] - (along * W[c, tile(s), :] - against * V[c, tile(s), :])
        return carry

    lax.fori_loop(0, groups, finish, 0)

    for t in range(3):
        sent(row_copies(t) + section_copies(t))
    sent((bits_copy, cross_copy))
    for copy in pending:
        copy.wait_send()


def tiles(shard):
    *lead, sections, nodes = shard.shape
    split = shard.reshape(*lead, sections // 8, 8, nodes // LANES, LANES)
    return jnp.swapaxes(split, -3, -2).reshape(*lead, sections * nodes // LANES, LANES)


def untiled(rows, sections, nodes):
    lead = rows.shape[:-2]
    split = rows.reshape(*lead, sections // 8, nodes // LANES, 8, LANES)
    return jnp.swapaxes(split, -3, -2).reshape(*lead, sections, nodes)


def per_device(n_gz, n_rows, forces, start, spring_bits, plane_stiffness, cross_weight, anchors):
    _, sections, nodes = forces.shape
    stages = stage_groups(n_gz, n_rows)
    f32 = functools.partial(pltpu.VMEM, dtype=jnp.float32)
    own, held = 8 * sections, 8 * (sections + 2 * PRED)
    scratch = [
        pltpu.SMEM((sections,), jnp.float32),
        pltpu.SMEM((PRED, sections), jnp.float32),
        pltpu.SMEM(anchors.shape, jnp.int32),
        f32((2, own, LANES)),
        f32((2, own, LANES)),
        pltpu.VMEM((own, LANES), jnp.int32),
        *[f32((2, held, LANES)) for _ in range(3)],
        *[f32((2, own, LANES)) for _ in range(5)],
        f32((3, own, LANES)),
        f32((6, own, LANES)),
        f32((PRED, own + 8 * PRED, LANES)),
        f32((sections, LANES)),
        f32((sections, LANES)),
        f32((3, 2, sections, LANES)),
        f32((3, sections, LANES)),
        f32((3, sections, LANES)),
        pltpu.VMEM((sections // 2, LANES), jnp.int32),
        pltpu.VMEM((sections // 2, LANES), jnp.int32),
        f32((4, sections, LANES)),
        *[f32((2, sections, LANES)) for _ in range(5)],
        *[f32((1, 1, LANES)) for _ in stages],
        *[f32((len(group), 1, LANES)) for group in stages],
        pltpu.SemaphoreType.DMA((6,)),
        pltpu.SemaphoreType.DMA((14,)),
        pltpu.SemaphoreType.DMA((14,)),
        pltpu.SemaphoreType.DMA((len(stages),)),
        pltpu.SemaphoreType.DMA((len(stages),)),
    ]
    shape = jax.ShapeDtypeStruct((2, own, LANES), jnp.float32)
    solved, left_over = pl.pallas_call(
        functools.partial(kernel, n_gz, n_rows, anchors.shape[0], stages),
        out_shape=(pltpu.VMEM(shape.shape, jnp.float32),) * 2,
        in_specs=[pl.BlockSpec(memory_space=pltpu.HBM)] * 6,
        out_specs=[pl.BlockSpec(memory_space=pltpu.VMEM)] * 2,
        scratch_shapes=scratch,
        compiler_params=pltpu.CompilerParams(
            collective_id=0, has_side_effects=True
        ),
        name="cg",
    )(tiles(forces), tiles(start), tiles(spring_bits), plane_stiffness, cross_weight, anchors)
    return untiled(solved, sections, nodes), untiled(left_over, sections, nodes)


def solution(mesh):
    return jax.shard_map(
        functools.partial(per_device, mesh.shape["gz"], mesh.shape["rows"]),
        mesh=mesh,
        in_specs=(P(None, "gz", "rows"), P(None, "gz", "rows"), P("gz", "rows"), P("gz"), P(None, "gz"), P()),
        out_specs=(P(None, "gz", "rows"), P(None, "gz", "rows")),
        check_vma=False,
    )
```

```python
import functools

import jax
import jax.numpy as jnp
from jax import lax
from jax.experimental import pallas as pl
from jax.experimental.pallas import tpu as pltpu
from jax.sharding import PartitionSpec as P

GRID = 64
PRED = 3
LANES = 128
APPLY_UNROLL = 18
FILL_UNROLL = 18
MESH = pl.DeviceIdType.MESH

damping = 0.05
anchor_stiffness = 20.0


def digit_sizes(size):
    return (4, 8, 2) if size == 64 else (1, size // 2, 2)


def stage_groups(size, rows):
    ny, nz, nc = digit_sizes(size)
    near = [(0, 0, c, x) for c in range(nc) for x in range(rows)][1:]
    far = [(y, z, 0, 0) for y in range(ny) for z in range(nz)][1:]
    return [group for group in (near, far) if group]


def kernel(
    n_gz, n_rows, n_anchors, stages,
    f_hbm, x_hbm, b_hbm, stiff_hbm, cross_hbm, anchors_hbm,
    out_x, out_r,
    stiff, cross, anchors,
    XS, FS, BS, X, Z, U, Y, W, V, R, INV, DG, WP, K, TE, KS,
    PS, HT, HB, BO, BT, PW, PI, PY, PH, PF, FX, *rest,
):
    n_stages = len(stages)
    totals_out, totals_in = rest[:n_stages], rest[n_stages : 2 * n_stages]
    load_sem, send_sem, recv_sem, tsend_sem, trecv_sem, word_sem = rest[2 * n_stages :]
    sections = TE.shape[0]
    groups = sections // 8
    g, r = lax.axis_index("gz"), lax.axis_index("rows")
    has_prev, has_next, has_above, has_below = g > 0, g < n_gz - 1, r > 0, r < n_rows - 1
    prev, nxt = {"gz": g - 1, "rows": r}, {"gz": g + 1, "rows": r}
    above, below = {"gz": g, "rows": r - 1}, {"gz": g, "rows": r + 1}

    loads = [
        pltpu.make_async_copy(src, dst, load_sem.at[i])
        for i, (src, dst) in enumerate(
            [(x_hbm, XS), (b_hbm, BS), (stiff_hbm, stiff), (cross_hbm, cross), (anchors_hbm, anchors), (f_hbm, FS)]
        )
    ]
    for load in loads:
        load.start()

    ny, nz, nc = digit_sizes(n_gz)
    my_digits = (g // (nz * nc), (g // nc) & (nz - 1), g & (nc - 1), r)

    def member(offset):
        y, z, c, x = [(d + o) & (n - 1) for d, o, n in zip(my_digits, offset, (ny, nz, nc, n_rows))]
        return {"gz": (y * nz + z) * nc + c, "rows": x}

    def steps(size, by):
        return sorted({step % size for step in by} - {0})

    beside = [(y, 0, 0, 0) for y in steps(ny, (1, -1))] + [(0, z, 0, 0) for z in steps(nz, (1, -1))]
    column_of = [(y, 0, 0, 0) for y in range(1, ny)]
    word = (beside, column_of + [(0, z, 0, 0) for z in steps(nz, (2, -2))], column_of)

    def say(t):
        for offset in word[t]:
            pl.semaphore_signal(word_sem.at[t], inc=1, device_id=member(offset), device_id_type=MESH)

    def hear(t):
        if word[t]:
            pl.semaphore_wait(word_sem.at[t], len(word[t]))

    barrier = pltpu.get_barrier_semaphore()
    for here, device in ((has_prev, prev), (has_next, nxt), (has_above, above), (has_below, below)):

        @pl.when(here)
        def _():
            pl.semaphore_signal(barrier, inc=1, device_id=device, device_id_type=MESH)

    greeted = stages[0] + beside
    for offset in greeted:
        pl.semaphore_signal(barrier, inc=1, device_id=member(offset), device_id_type=MESH)

    lane = lax.broadcasted_iota(jnp.int32, (8, LANES), 1)
    sub = lax.broadcasted_iota(jnp.int32, (8, LANES), 0)
    lo = lane < GRID
    column = lane % GRID
    open_column = column < GRID - 1
    inner_row = (2 * sub + lane // GRID) < 15
    mask_right = jnp.where(open_column, 1, 0)
    mask_down = jnp.where(inner_row, 2, 0)
    mask_diag = jnp.where(open_column & inner_row, 4, 0)
    down_scale = jnp.where(lo, 0.25, 1.0).astype(jnp.float32)
    zero = jnp.zeros((8, LANES), jnp.float32)

    def half(v):
        return pltpu.roll(v, GRID, 1)

    def left(v):
        return pltpu.roll(v, LANES - 1, 1)

    def right(v):
        return pltpu.roll(v, 1, 1)

    def lowered(v, by):
        return pltpu.roll(jnp.where(lo, v, pltpu.roll(v, 1, 0)), by, 1)

    def tile(s):
        return pl.ds(pl.multiple_of(8 * s, 8), 8)

    def raw(s):
        return pl.ds((s // 8) * 64 + s % 8, 8, stride=8)

    def pack_last(a, b):
        return jnp.where(lo, half(a), b)

    def pack_first(a, b):
        return jnp.where(lo, a, half(b))

    base = g * sections

    def cross_weights(s):
        bits = BS[raw(s), :]
        KS[pl.ds(s, 1), :] = jnp.full((1, LANES), stiff[s], jnp.float32)
        for j in range(PRED):
            kj = jnp.where(base + s > j, cross[j, s], 0.0)
            K[j, tile(s), :] = jnp.where((bits & (8 << j)) != 0, jnp.full((8, LANES), kj, jnp.float32), zero)
        return bits

    def plane_weights(s, bits):
        k = jnp.full((8, LANES), stiff[s], jnp.float32)
        wr = jnp.where((bits & mask_right) != 0, k, zero)
        wd = jnp.where((bits & mask_down) != 0, k, zero)
        wg = jnp.where((bits & mask_diag) != 0, k, zero)
        for n, w in enumerate((wr, right(wr), wd, lowered(wd, GRID), wg, lowered(wg, GRID + 1))):
            WP[n, tile(s), :] = w

    for load in loads[1:4]:
        load.wait()
    for s in range(PRED):
        cross_weights(s)

    for q in range(groups // 2):
        a = BS[64 * q + 56 : 64 * q + 64, :]
        b = BS[64 * (q + groups // 2) + 56 : 64 * (q + groups // 2) + 64, :]
        BO[8 * q : 8 * q + 8, :] = jnp.where(lo, half(a), b)

    loads[0].wait()
    for c in range(2):
        for s in list(range(PRED)) + list(range(sections - PRED, sections)):
            X[c, 8 * (s + PRED) : 8 * (s + PRED) + 8, :] = XS[c, pl.ds((s // 8) * 64 + s % 8, 8, stride=8), :]
    for q in range(groups):
        rows = slice(8 * q, 8 * q + 8)
        PS[0, 0, rows, :] = pack_first(XS[0, 64 * q : 64 * q + 8, :], XS[1, 64 * q : 64 * q + 8, :])
        PS[0, 1, rows, :] = pack_last(XS[0, 64 * q + 56 : 64 * q + 64, :], XS[1, 64 * q + 56 : 64 * q + 64, :])

    near = sum(jnp.where(here, 1, 0) for here in (has_prev, has_next, has_above, has_below))
    pl.semaphore_wait(barrier, near + len(greeted))

    def remote(src, dst, at, device):
        return pltpu.make_async_remote_copy(
            src_ref=src, dst_ref=dst, send_sem=send_sem.at[at], recv_sem=recv_sem.at[at],
            device_id=device, device_id_type=MESH,
        )

    edge = 8 * PRED
    own = 8 * sections

    def row_copies(t):
        return (
            (has_below, has_above, remote(PS.at[t, 1], HT.at[t], 4 * t, below)),
            (has_above, has_below, remote(PS.at[t, 0], HB.at[t], 4 * t + 1, above)),
        )

    def section_copies(t):
        v = (X, Z, U)[t]
        return (
            (has_next, has_prev, remote(v.at[:, pl.ds(own, edge)], v.at[:, pl.ds(0, edge)], 4 * t + 2, nxt)),
            (has_prev, has_next, remote(v.at[:, pl.ds(edge, edge)], v.at[:, pl.ds(own + edge, edge)], 4 * t + 3, prev)),
        )

    bits_copy = (has_below, has_above, remote(BO, BT, 12, below))
    cross_copy = (has_prev, has_next, remote(K.at[:, pl.ds(0, edge)], K.at[:, pl.ds(own, edge)], 13, prev))

    def start(copies):
        for sends, _, copy in copies:
            pl.when(sends)(copy.start)

    def arrive(copies):
        for _, receives, copy in copies:
            pl.when(receives)(copy.wait_recv)

    def sent(copies):
        for sends, _, copy in copies:
            pl.when(sends)(copy.wait_send)

    start(row_copies(0) + section_copies(0) + (cross_copy, bits_copy))
    say(0)

    loads[4].wait()

    def anchor_step(i, hits):
        a = anchors[i] - base
        return tuple(jnp.where(sub + 8 * q == a, 1, hit) for q, hit in enumerate(hits))

    hits = lax.fori_loop(0, n_anchors, anchor_step, tuple(jnp.zeros((8, LANES), jnp.int32) for _ in range(groups)))
    for q in range(groups):
        TE[8 * q : 8 * q + 8, :] = jnp.where(hits[q] > 0, damping + anchor_stiffness, damping).astype(jnp.float32)

    wide = jnp.zeros((2, edge, LANES), jnp.float32)

    @pl.when(jnp.logical_not(has_prev))
    def _():
        for v in (X, Z, U):
            v[:, 0:edge, :] = wide

    @pl.when(jnp.logical_not(has_next))
    def _():
        for v in (X, Z, U):
            v[:, own + edge : own + 2 * edge, :] = wide
        K[:, own : own + edge, :] = jnp.zeros((PRED, edge, LANES), jnp.float32)

    @pl.when(jnp.logical_not(has_above))
    def _():
        HT[...] = jnp.zeros(HT.shape, jnp.float32)
        BT[...] = jnp.zeros(BT.shape, jnp.int32)

    @pl.when(jnp.logical_not(has_below))
    def _():
        HB[...] = jnp.zeros(HB.shape, jnp.float32)

    ends = list(range(PRED)) + list(range(sections - PRED, sections))
    inner = sections - 2 * PRED

    def over_inner(body, carry, most):
        unroll = next(n for n in range(most, 0, -1) if inner % n == 0)

        def step(i, carry):
            for n in range(unroll):
                carry = body(PRED + unroll * i + n, carry)
            return carry

        return lax.fori_loop(0, inner // unroll, step, carry)

    def fill(s, carry):
        plane_weights(s, cross_weights(s))
        for c in range(2):
            X[c, tile(s + PRED), :] = XS[c, raw(s), :]
        return carry

    over_inner(fill, 0, FILL_UNROLL)
    for s in range(PRED):
        plane_weights(s, BS[raw(s), :])
    for s in range(sections - PRED, sections):
        plane_weights(s, cross_weights(s))

    def apply(v, out, s, first=False):
        wr, wl, wd, wu, wg, wv = [WP[n, tile(s), :] for n in range(6)]
        back = [K[j, tile(s), :] for j in range(PRED)]
        ahead = [K[j, tile(s + j + 1), :] for j in range(PRED)]
        if first:
            tether = jnp.broadcast_to(TE[pl.ds(s, 1), :], (8, LANES))
            shared = tether + ((back[0] + ahead[0]) + (back[1] + ahead[1]) + (back[2] + ahead[2]))
            shared = shared + 0.625 * (wg + wv)
            across, along = wr + wl, wd + wu
            own_weight = [shared + across + 0.25 * along, shared + 0.25 * across + along]
            mixed = 0.375 * (wg + wv)
            DG[2, tile(s), :] = mixed
            for c in range(2):
                DG[c, tile(s), :] = own_weight[c]
                INV[c, tile(s), :] = 1.0 / own_weight[c]
        else:
            own_weight, mixed = [DG[c, tile(s), :] for c in range(2)], DG[2, tile(s), :]
        mine = [v[c, tile(s + PRED), :] for c in range(2)]
        sides, lines, slants = [], [], []
        for c in range(2):
            after = jnp.where(lo, v[c, pl.ds(8 * (s + PRED) + 1, 8), :], mine[c])
            before = jnp.where(lo, mine[c], v[c, pl.ds(8 * (s + PRED) - 1, 8), :])
            sides.append(wr * left(mine[c]) + wl * right(mine[c]))
            lines.append(wd * half(after) + wu * half(before))
            slants.append(wg * pltpu.roll(after, GRID - 1, 1) + wv * pltpu.roll(before, GRID + 1, 1))
        pulls = [
            (sides[0] + 0.25 * lines[0]) + (0.625 * slants[0] + 0.375 * slants[1]),
            (0.25 * sides[1] + lines[1]) + (0.375 * slants[0] + 0.625 * slants[1]),
        ]
        done = []
        for c in range(2):
            ties = [
                back[j] * v[c, tile(s + PRED - j - 1), :] + ahead[j] * v[c, tile(s + PRED + j + 1), :]
                for j in range(PRED)
            ]
            total = (own_weight[c] * mine[c] + mixed * mine[1 - c]) - (pulls[c] + (ties[0] + ties[1] + ties[2]))
            out[c, tile(s), :] = total
            done.append(total)
        return mine[0] * done[0] + mine[1] * done[1]

    def first_apply(s, carry):
        apply(X, Y, s, first=True)
        return carry

    over_inner(first_apply, 0, APPLY_UNROLL)

    def rows_of(q):
        return slice(8 * q, 8 * q + 8)

    def packed(ref, q):
        at = [[ref[c, pl.ds(64 * q + line, 8, stride=8), :] for c in range(2)] for line in (0, 7)]
        return pack_first(*at[0]), pack_last(*at[1])

    def spread(top, bottom):
        return (top, half(top)), (half(bottom), bottom)

    def change_rows(ref, q, top, bottom, change):
        for line, keep_lo, parts in zip((0, 7), (False, True), spread(top, bottom)):
            for c in range(2):
                to = pl.ds(64 * q + line, 8, stride=8)
                old = ref[c, to, :]
                new = change(old, parts[c])
                ref[c, to, :] = jnp.where(lo, old, new) if keep_lo else jnp.where(lo, new, old)

    for q in range(groups):
        rows = rows_of(q)
        bits = BS[64 * q + 56 : 64 * q + 64, :]
        bits = jnp.where(lo, half(bits), bits)
        k = jnp.where(has_below, KS[rows, :], zero)
        PW[2, rows, :] = jnp.where((bits & 2) != 0, k, zero) * down_scale
        PW[3, rows, :] = jnp.where(((bits & 4) != 0) & open_column, k, zero)

    middle = range(1, groups - 1)
    outer = sorted({0, groups - 1})

    def before_rows(t, out, some):
        for q in some:
            rows = rows_of(q)
            for n, part in enumerate(packed(out, q)):
                PY[n, rows, :] = part
                PH[n, rows, :] = half(PS[t, n, rows, :])

    def outside(t, q):
        rows = rows_of(q)
        mine, turned, other = PS[t, 0, rows, :], PH[0, rows, :], HT[t, rows, :]
        slant = 0.625 * (right(other) - mine) + 0.375 * (pltpu.roll(other, GRID + 1, 1) - turned)
        top = PW[0, rows, :] * (mine - other) - PW[1, rows, :] * slant
        mine, turned, other = PS[t, 1, rows, :], PH[1, rows, :], HB[t, rows, :]
        slant = 0.625 * (mine - left(other)) + 0.375 * (turned - pltpu.roll(other, GRID - 1, 1))
        bottom = PW[2, rows, :] * (mine - other) + PW[3, rows, :] * slant
        FX[0, rows, :] = top
        FX[1, rows, :] = bottom
        return top, bottom

    def add(old, new):
        return old + new

    def put(old, new):
        return new

    before_rows(0, Y, middle)
    loads[5].wait()
    for q in range(groups):
        rows = rows_of(q)
        head, foot = slice(64 * q, 64 * q + 8), slice(64 * q + 56, 64 * q + 64)
        PF[0, rows, :] = pack_first(FS[0, head, :], FS[1, head, :])
        PF[1, rows, :] = pack_last(FS[0, foot, :], FS[1, foot, :])

    arrive((cross_copy,) + section_copies(0) + row_copies(0) + (bits_copy,))
    hear(0)
    for q in range(groups // 2):
        both = BT[rows_of(q), :]
        for n, bits in enumerate((jnp.where(lo, both, half(both)), jnp.where(lo, half(both), both))):
            rows = rows_of(q + n * (groups // 2))
            k = jnp.where(has_above, KS[rows, :], zero)
            PW[0, rows, :] = jnp.where((bits & 2) != 0, k, zero) * down_scale
            PW[1, rows, :] = right(jnp.where(((bits & 4) != 0) & open_column, k, zero))

    for s in ends:
        first_apply(s, 0)
    before_rows(0, Y, outer)
    for q in range(groups):
        rows = rows_of(q)
        top, bottom = packed(DG, q)
        PI[0, rows, :] = 1.0 / (top + (PW[0, rows, :] + 0.625 * PW[1, rows, :]))
        PI[1, rows, :] = 1.0 / (bottom + (PW[2, rows, :] + 0.625 * PW[3, rows, :]))
    for q in range(groups):
        rows = rows_of(q)
        for n, part in enumerate(outside(0, q)):
            res = PF[n, rows, :] - (PY[n, rows, :] + part)
            PF[n, rows, :] = res
            PS[1, n, rows, :] = res * PI[n, rows, :]
    start(row_copies(1))
    say(1)
    for q in range(groups):
        rows = rows_of(q)
        change_rows(Y, q, FX[0, rows, :], FX[1, rows, :], add)
        change_rows(INV, q, PI[0, rows, :], PI[1, rows, :], put)

    def residual(s, total):
        for c in range(2):
            res = FS[c, raw(s), :] - Y[c, tile(s), :]
            pre = res * INV[c, tile(s), :]
            R[c, tile(s), :] = res
            Z[c, tile(s + PRED), :] = pre
            total = total + res * pre
        return total

    sum0 = zero
    for s in ends:
        sum0 = residual(s, sum0)
    start(section_copies(1))
    sum0 = over_inner(residual, sum0, 10)

    def second_apply(s, carry):
        apply(Z, W, s)
        return carry

    over_inner(second_apply, 0, APPLY_UNROLL)
    before_rows(1, W, middle)

    arrive(section_copies(1) + row_copies(1))
    hear(1)
    for s in ends:
        second_apply(s, 0)
    before_rows(1, W, outer)
    for q in range(groups):
        rows = rows_of(q)
        for n, part in enumerate(outside(1, q)):
            PS[2, n, rows, :] = (PF[n, rows, :] - (PY[n, rows, :] + part)) * PI[n, rows, :]
    start(row_copies(2))
    say(2)
    for q in range(groups):
        change_rows(W, q, FX[0, rows_of(q), :], FX[1, rows_of(q), :], add)

    def second(s, totals):
        sum1, sum2 = totals
        for c in range(2):
            gap = R[c, tile(s), :] - W[c, tile(s), :]
            u = gap * INV[c, tile(s), :]
            U[c, tile(s + PRED), :] = u
            sum1 = sum1 + gap * Z[c, tile(s + PRED), :]
            sum2 = sum2 + gap * u
        return sum1, sum2

    sums = (zero, zero)
    for s in ends:
        sums = second(s, sums)
    start(section_copies(2))
    sum1, sum2 = over_inner(second, sums, 10)
    sum3 = over_inner(lambda s, total: total + apply(U, V, s), zero, APPLY_UNROLL)
    for q in range(groups):
        for n in range(2):
            PH[n, rows_of(q), :] = half(PS[2, n, rows_of(q), :])

    arrive(section_copies(2) + row_copies(2))
    hear(2)
    for s in ends:
        sum3 = sum3 + apply(U, V, s)
    for q in range(groups):
        top, bottom = outside(2, q)
        sum3 = sum3 + (top * PS[2, 0, rows_of(q), :] + bottom * PS[2, 1, rows_of(q), :])

    row = zero
    for n, part in enumerate((sum0, sum1, sum2, sum3)):
        part = part + half(part)
        part = part + pltpu.roll(part, 32, 1)
        row = jnp.where(lane // 32 == n, part, row)
    row = jnp.sum(row, axis=0, keepdims=True)
    pending = []

    def finish_rows():
        for q in range(groups):
            change_rows(V, q, FX[0, rows_of(q), :], FX[1, rows_of(q), :], add)

    for t, group in enumerate(stages):
        totals_out[t][0] = row
        for n, offset in enumerate(group):
            copy = pltpu.make_async_remote_copy(
                src_ref=totals_out[t].at[0], dst_ref=totals_in[t].at[n],
                send_sem=tsend_sem.at[t], recv_sem=trecv_sem.at[t],
                device_id=member(offset), device_id_type=MESH,
            )
            copy.start()
        everyone = pltpu.make_async_remote_copy(
            src_ref=totals_in[t], dst_ref=totals_in[t], send_sem=tsend_sem.at[t], recv_sem=trecv_sem.at[t],
            device_id=member(group[0]), device_id_type=MESH,
        )
        if t == 0:
            finish_rows()
        everyone.wait_recv()
        pending.append(everyone)
        row = row + jnp.sum(totals_in[t][...], axis=0)

    lanes = lax.broadcasted_iota(jnp.int32, (1, LANES), 1) // 32
    zz, zy, yy, ay = [jnp.sum(jnp.where(lanes == n, row, 0.0), axis=1, keepdims=True) for n in range(4)]
    curve = zz - zy
    alpha0 = zz / curve
    turn = -zy / curve
    inner1 = alpha0 * alpha0 * (yy - zy * zy / zz)
    growth = inner1 / zz
    bend = turn * turn * curve + 2.0 * turn * alpha0 * (zy - yy) + alpha0 * alpha0 * ay
    alpha1 = inner1 / (bend - growth * inner1 / alpha0)
    along = jnp.broadcast_to(alpha0 + alpha1 * (turn + growth), (8, LANES))
    across = jnp.broadcast_to(alpha1 * alpha0, (8, LANES))

    def finish(q, carry):
        for n in range(8):
            s = 8 * q + n
            for c in range(2):
                to = pl.ds(64 * q + n, 8, stride=8)
                z, u = Z[c, tile(s + PRED), :], U[c, tile(s + PRED), :]
                out_x[c, to, :] = X[c, tile(s + PRED), :] + (along * z + across * u)
                out_r[c, to, :] = R[c, tile(s), :] - (along * W[c, tile(s), :] + across * V[c, tile(s), :])
        return carry

    lax.fori_loop(0, groups, finish, 0)

    for t in range(3):
        sent(row_copies(t) + section_copies(t))
    sent((bits_copy, cross_copy))
    for copy in pending:
        copy.wait_send()


def tiles(shard):
    *lead, sections, nodes = shard.shape
    split = shard.reshape(*lead, sections // 8, 8, nodes // LANES, LANES)
    return jnp.swapaxes(split, -3, -2).reshape(*lead, sections * nodes // LANES, LANES)


def untiled(rows, sections, nodes):
    lead = rows.shape[:-2]
    split = rows.reshape(*lead, sections // 8, nodes // LANES, 8, LANES)
    return jnp.swapaxes(split, -3, -2).reshape(*lead, sections, nodes)


def per_device(n_gz, n_rows, forces, start, spring_bits, plane_stiffness, cross_weight, anchors):
    _, sections, nodes = forces.shape
    stages = stage_groups(n_gz, n_rows)
    f32 = functools.partial(pltpu.VMEM, dtype=jnp.float32)
    own, held = 8 * sections, 8 * (sections + 2 * PRED)
    scratch = [
        pltpu.SMEM((sections,), jnp.float32),
        pltpu.SMEM((PRED, sections), jnp.float32),
        pltpu.SMEM(anchors.shape, jnp.int32),
        f32((2, own, LANES)),
        f32((2, own, LANES)),
        pltpu.VMEM((own, LANES), jnp.int32),
        *[f32((2, held, LANES)) for _ in range(3)],
        *[f32((2, own, LANES)) for _ in range(5)],
        f32((3, own, LANES)),
        f32((6, own, LANES)),
        f32((PRED, own + 8 * PRED, LANES)),
        f32((sections, LANES)),
        f32((sections, LANES)),
        f32((3, 2, sections, LANES)),
        f32((3, sections, LANES)),
        f32((3, sections, LANES)),
        pltpu.VMEM((sections // 2, LANES), jnp.int32),
        pltpu.VMEM((sections // 2, LANES), jnp.int32),
        f32((4, sections, LANES)),
        *[f32((2, sections, LANES)) for _ in range(5)],
        *[f32((1, 1, LANES)) for _ in stages],
        *[f32((len(group), 1, LANES)) for group in stages],
        pltpu.SemaphoreType.DMA((6,)),
        pltpu.SemaphoreType.DMA((14,)),
        pltpu.SemaphoreType.DMA((14,)),
        pltpu.SemaphoreType.DMA((len(stages),)),
        pltpu.SemaphoreType.DMA((len(stages),)),
        pltpu.SemaphoreType.REGULAR((3,)),
    ]
    shape = jax.ShapeDtypeStruct((2, own, LANES), jnp.float32)
    solved, left_over = pl.pallas_call(
        functools.partial(kernel, n_gz, n_rows, anchors.shape[0], stages),
        out_shape=(pltpu.VMEM(shape.shape, jnp.float32),) * 2,
        in_specs=[pl.BlockSpec(memory_space=pltpu.HBM)] * 6,
        out_specs=[pl.BlockSpec(memory_space=pltpu.VMEM)] * 2,
        scratch_shapes=scratch,
        compiler_params=pltpu.CompilerParams(
            collective_id=0, has_side_effects=True
        ),
        name="cg",
    )(tiles(forces), tiles(start), tiles(spring_bits), plane_stiffness, cross_weight, anchors)
    return untiled(solved, sections, nodes), untiled(left_over, sections, nodes)


def solution(mesh):
    return jax.shard_map(
        functools.partial(per_device, mesh.shape["gz"], mesh.shape["rows"]),
        mesh=mesh,
        in_specs=(P(None, "gz", "rows"), P(None, "gz", "rows"), P("gz", "rows"), P("gz"), P(None, "gz"), P()),
        out_specs=(P(None, "gz", "rows"), P(None, "gz", "rows")),
        check_vma=False,
    )
```

```python
import functools

import jax
import jax.numpy as jnp
from jax import lax
from jax.experimental import pallas as pl
from jax.experimental.pallas import tpu as pltpu
from jax.sharding import PartitionSpec as P

GRID = 64
PRED = 3
LANES = 128
PARTS = 3
APPLY_UNROLL = 18
FILL_UNROLL = 18
MESH = pl.DeviceIdType.MESH

damping = 0.05
anchor_stiffness = 20.0


def digit_sizes(size):
    return (4, 8, 2) if size == 64 else (1, size // 2, 2)


def stage_groups(size, rows):
    ny, nz, nc = digit_sizes(size)
    twin = [(0, 0, c, 0) for c in range(1, nc)]
    rest = [(y, z, 0, x) for y in range(ny) for z in range(nz) for x in range(rows)][1:]

    def hops(offset):
        return sum(min(d, n - d) for d, n in zip(offset, (ny, nz, nc, rows)))

    return [sorted(group, key=hops, reverse=True) for group in (twin, rest) if group]


def kernel(
    n_gz, n_rows, n_anchors, stages,
    f_hbm, x_hbm, b_hbm, stiff_hbm, cross_hbm, anchors_hbm,
    X, Z, U, R, W, V, factors,
    stiff, cross, anchors,
    XS, FS, BS, Y, INV, DG, WP, K, TE, KS,
    PS, HT, HB, BO, BT, PW, PI, PY, PH, PF, FX, *rest,
):
    n_stages = len(stages)
    totals_out, totals_in = rest[:n_stages], rest[n_stages : 2 * n_stages]
    load_sem, send_sem, recv_sem, tsend_sem, trecv_sem, word_sem = rest[2 * n_stages :]
    sections = TE.shape[0]
    groups = sections // 8
    g, r = lax.axis_index("gz"), lax.axis_index("rows")
    has_prev, has_next, has_above, has_below = g > 0, g < n_gz - 1, r > 0, r < n_rows - 1
    prev, nxt = {"gz": g - 1, "rows": r}, {"gz": g + 1, "rows": r}
    above, below = {"gz": g, "rows": r - 1}, {"gz": g, "rows": r + 1}

    loads = [
        pltpu.make_async_copy(src, dst, load_sem.at[i])
        for i, (src, dst) in enumerate(
            [(anchors_hbm, anchors), (stiff_hbm, stiff), (cross_hbm, cross), (b_hbm, BS), (x_hbm, XS), (f_hbm, FS)]
        )
    ]
    for load in loads[:5]:
        load.start()

    ny, nz, nc = digit_sizes(n_gz)
    my_digits = (g // (nz * nc), (g // nc) & (nz - 1), g & (nc - 1), r)

    def member(offset):
        y, z, c, x = [(d + o) & (n - 1) for d, o, n in zip(my_digits, offset, (ny, nz, nc, n_rows))]
        return {"gz": (y * nz + z) * nc + c, "rows": x}

    def steps(size, by):
        return sorted({step % size for step in by} - {0})

    beside = [(y, 0, 0, 0) for y in steps(ny, (1, -1))] + [(0, 0, 0, x) for x in steps(n_rows, (1, -1))]
    beside += [(0, z, 0, 0) for z in steps(nz, (1, -1, 2, -2))]
    word = (beside, [(0, 0, 0, x) for x in range(1, n_rows)], [(y, 0, 0, 0) for y in range(1, ny)])

    def say(t):
        for offset in word[t]:
            pl.semaphore_signal(word_sem.at[t], inc=1, device_id=member(offset), device_id_type=MESH)

    def hear(t):
        if word[t]:
            pl.semaphore_wait(word_sem.at[t], len(word[t]))

    barrier = pltpu.get_barrier_semaphore()
    for here, device in ((has_prev, prev), (has_next, nxt), (has_above, above), (has_below, below)):

        @pl.when(here)
        def _():
            pl.semaphore_signal(barrier, inc=1, device_id=device, device_id_type=MESH)

    greeted = stages[0] + beside
    for offset in greeted:
        pl.semaphore_signal(barrier, inc=1, device_id=member(offset), device_id_type=MESH)

    lane = lax.broadcasted_iota(jnp.int32, (8, LANES), 1)
    sub = lax.broadcasted_iota(jnp.int32, (8, LANES), 0)
    lo = lane < GRID
    column = lane % GRID
    open_column = column < GRID - 1
    inner_row = (2 * sub + lane // GRID) < 15
    mask_right = jnp.where(open_column, 1, 0)
    mask_down = jnp.where(inner_row, 2, 0)
    mask_diag = jnp.where(open_column & inner_row, 4, 0)
    down_scale = jnp.where(lo, 0.25, 1.0).astype(jnp.float32)
    zero = jnp.zeros((8, LANES), jnp.float32)

    def half(v):
        return pltpu.roll(v, GRID, 1)

    def left(v):
        return pltpu.roll(v, LANES - 1, 1)

    def right(v):
        return pltpu.roll(v, 1, 1)

    def lowered(v, by):
        return pltpu.roll(jnp.where(lo, v, pltpu.roll(v, 1, 0)), by, 1)

    def tile(s):
        return pl.ds(pl.multiple_of(8 * s, 8), 8)

    def raw(s):
        return pl.ds((s // 8) * 64 + s % 8, 8, stride=8)

    def pack_last(a, b):
        return jnp.where(lo, half(a), b)

    def pack_first(a, b):
        return jnp.where(lo, a, half(b))

    base = g * sections

    loads[0].wait()

    def anchor_step(i, hits):
        for n in range(8):
            a = anchors[8 * i + n] - base
            hits = tuple(jnp.where(sub == a - 8 * q, 1, hit) for q, hit in enumerate(hits))
        return hits

    hits = lax.fori_loop(0, n_anchors // 8, anchor_step, tuple(jnp.zeros((8, LANES), jnp.int32) for _ in range(groups)))
    for q in range(groups):
        TE[8 * q : 8 * q + 8, :] = jnp.where(hits[q] > 0, damping + anchor_stiffness, damping).astype(jnp.float32)

    def cross_weights(s):
        bits = BS[raw(s), :]
        KS[pl.ds(s, 1), :] = jnp.full((1, LANES), stiff[s], jnp.float32)
        for j in range(PRED):
            kj = jnp.where(base + s > j, cross[j, s], 0.0)
            K[j, tile(s), :] = jnp.where((bits & (8 << j)) != 0, jnp.full((8, LANES), kj, jnp.float32), zero)
        return bits

    def plane_weights(s, bits):
        k = jnp.full((8, LANES), stiff[s], jnp.float32)
        wr = jnp.where((bits & mask_right) != 0, k, zero)
        wd = jnp.where((bits & mask_down) != 0, k, zero)
        wg = jnp.where((bits & mask_diag) != 0, k, zero)
        for n, w in enumerate((wr, right(wr), wd, lowered(wd, GRID), wg, lowered(wg, GRID + 1))):
            WP[n, tile(s), :] = w

    for load in loads[1:4]:
        load.wait()
    for s in range(PRED):
        cross_weights(s)

    for q in range(groups // 2):
        a = BS[64 * q + 56 : 64 * q + 64, :]
        b = BS[64 * (q + groups // 2) + 56 : 64 * (q + groups // 2) + 64, :]
        BO[8 * q : 8 * q + 8, :] = jnp.where(lo, half(a), b)

    loads[4].wait()
    for c in range(2):
        for s in list(range(PRED)) + list(range(sections - PRED, sections)):
            X[c, 8 * (s + PRED) : 8 * (s + PRED) + 8, :] = XS[c, pl.ds((s // 8) * 64 + s % 8, 8, stride=8), :]
    for q in range(groups):
        rows = slice(8 * q, 8 * q + 8)
        PS[0, 0, rows, :] = pack_first(XS[0, 64 * q : 64 * q + 8, :], XS[1, 64 * q : 64 * q + 8, :])
        PS[0, 1, rows, :] = pack_last(XS[0, 64 * q + 56 : 64 * q + 64, :], XS[1, 64 * q + 56 : 64 * q + 64, :])

    near = sum(jnp.where(here, 1, 0) for here in (has_prev, has_next, has_above, has_below))
    pl.semaphore_wait(barrier, near + len(greeted))

    def remote(src, dst, at, device):
        return pltpu.make_async_remote_copy(
            src_ref=src, dst_ref=dst, send_sem=send_sem.at[at], recv_sem=recv_sem.at[at],
            device_id=device, device_id_type=MESH,
        )

    edge = 8 * PRED
    own = 8 * sections

    def row_copies(t):
        return (
            (has_below, has_above, remote(PS.at[t, 1], HT.at[t], 4 * t, below)),
            (has_above, has_below, remote(PS.at[t, 0], HB.at[t], 4 * t + 1, above)),
        )

    def section_copies(t):
        v = (X, Z, U)[t]
        return (
            (has_next, has_prev, remote(v.at[:, pl.ds(own, edge)], v.at[:, pl.ds(0, edge)], 4 * t + 2, nxt)),
            (has_prev, has_next, remote(v.at[:, pl.ds(edge, edge)], v.at[:, pl.ds(own + edge, edge)], 4 * t + 3, prev)),
        )

    bits_copy = (has_below, has_above, remote(BO, BT, 12, below))
    cross_copy = (has_prev, has_next, remote(K.at[:, pl.ds(0, edge)], K.at[:, pl.ds(own, edge)], 13, prev))

    def start(copies):
        for sends, _, copy in copies:
            pl.when(sends)(copy.start)

    def arrive(copies):
        for _, receives, copy in copies:
            pl.when(receives)(copy.wait_recv)

    def sent(copies):
        for sends, _, copy in copies:
            pl.when(sends)(copy.wait_send)

    start(row_copies(0) + section_copies(0) + (cross_copy, bits_copy))
    loads[5].start()
    say(0)

    wide = jnp.zeros((2, edge, LANES), jnp.float32)

    @pl.when(jnp.logical_not(has_prev))
    def _():
        for v in (X, Z, U):
            v[:, 0:edge, :] = wide

    @pl.when(jnp.logical_not(has_next))
    def _():
        for v in (X, Z, U):
            v[:, own + edge : own + 2 * edge, :] = wide
        K[:, own : own + edge, :] = jnp.zeros((PRED, edge, LANES), jnp.float32)

    @pl.when(jnp.logical_not(has_above))
    def _():
        HT[...] = jnp.zeros(HT.shape, jnp.float32)
        BT[...] = jnp.zeros(BT.shape, jnp.int32)

    @pl.when(jnp.logical_not(has_below))
    def _():
        HB[...] = jnp.zeros(HB.shape, jnp.float32)

    ends = list(range(PRED)) + list(range(sections - PRED, sections))
    inner = sections - 2 * PRED

    def over_inner(body, carry, most):
        unroll = next(n for n in range(most, 0, -1) if inner % n == 0)

        def step(i, carry):
            for n in range(unroll):
                carry = body(PRED + unroll * i + n, carry)
            return carry

        return lax.fori_loop(0, inner // unroll, step, carry)

    def fill(s, carry):
        plane_weights(s, cross_weights(s))
        for c in range(2):
            X[c, tile(s + PRED), :] = XS[c, raw(s), :]
        return carry

    over_inner(fill, 0, FILL_UNROLL)
    for s in range(PRED):
        plane_weights(s, BS[raw(s), :])
    for s in range(sections - PRED, sections):
        plane_weights(s, cross_weights(s))

    def apply(v, out, s, first=False):
        wr, wl, wd, wu, wg, wv = [WP[n, tile(s), :] for n in range(6)]
        back = [K[j, tile(s), :] for j in range(PRED)]
        ahead = [K[j, tile(s + j + 1), :] for j in range(PRED)]
        if first:
            tether = jnp.broadcast_to(TE[pl.ds(s, 1), :], (8, LANES))
            shared = tether + ((back[0] + ahead[0]) + (back[1] + ahead[1]) + (back[2] + ahead[2]))
            shared = shared + 0.625 * (wg + wv)
            across, along = wr + wl, wd + wu
            own_weight = [shared + across + 0.25 * along, shared + 0.25 * across + along]
            mixed = 0.375 * (wg + wv)
            DG[2, tile(s), :] = mixed
            for c in range(2):
                DG[c, tile(s), :] = own_weight[c]
                INV[c, tile(s), :] = 1.0 / own_weight[c]
        else:
            own_weight, mixed = [DG[c, tile(s), :] for c in range(2)], DG[2, tile(s), :]
        mine = [v[c, tile(s + PRED), :] for c in range(2)]
        sides, lines, slants = [], [], []
        for c in range(2):
            after = jnp.where(lo, v[c, pl.ds(8 * (s + PRED) + 1, 8), :], mine[c])
            before = jnp.where(lo, mine[c], v[c, pl.ds(8 * (s + PRED) - 1, 8), :])
            sides.append(wr * left(mine[c]) + wl * right(mine[c]))
            lines.append(wd * half(after) + wu * half(before))
            slants.append(wg * pltpu.roll(after, GRID - 1, 1) + wv * pltpu.roll(before, GRID + 1, 1))
        pulls = [
            (sides[0] + 0.25 * lines[0]) + (0.625 * slants[0] + 0.375 * slants[1]),
            (0.25 * sides[1] + lines[1]) + (0.375 * slants[0] + 0.625 * slants[1]),
        ]
        done = []
        for c in range(2):
            ties = [
                back[j] * v[c, tile(s + PRED - j - 1), :] + ahead[j] * v[c, tile(s + PRED + j + 1), :]
                for j in range(PRED)
            ]
            total = (own_weight[c] * mine[c] + mixed * mine[1 - c]) - (pulls[c] + (ties[0] + ties[1] + ties[2]))
            out[c, tile(s), :] = total
            done.append(total)
        return mine[0] * done[0] + mine[1] * done[1]

    def first_apply(s, carry):
        apply(X, Y, s, first=True)
        return carry

    over_inner(first_apply, 0, APPLY_UNROLL)

    def rows_of(q):
        return slice(8 * q, 8 * q + 8)

    def packed(ref, q):
        at = [[ref[c, pl.ds(64 * q + line, 8, stride=8), :] for c in range(2)] for line in (0, 7)]
        return pack_first(*at[0]), pack_last(*at[1])

    def spread(top, bottom):
        return (top, half(top)), (half(bottom), bottom)

    def change_rows(ref, q, top, bottom, change):
        for line, keep_lo, parts in zip((0, 7), (False, True), spread(top, bottom)):
            for c in range(2):
                to = pl.ds(64 * q + line, 8, stride=8)
                old = ref[c, to, :]
                new = change(old, parts[c])
                ref[c, to, :] = jnp.where(lo, old, new) if keep_lo else jnp.where(lo, new, old)

    for q in range(groups):
        rows = rows_of(q)
        bits = BS[64 * q + 56 : 64 * q + 64, :]
        bits = jnp.where(lo, half(bits), bits)
        k = jnp.where(has_below, KS[rows, :], zero)
        PW[2, rows, :] = jnp.where((bits & 2) != 0, k, zero) * down_scale
        PW[3, rows, :] = jnp.where(((bits & 4) != 0) & open_column, k, zero)

    middle = range(1, groups - 1)
    outer = sorted({0, groups - 1})

    def before_rows(t, out, some):
        for q in some:
            rows = rows_of(q)
            for n, part in enumerate(packed(out, q)):
                PY[n, rows, :] = part
                PH[n, rows, :] = half(PS[t, n, rows, :])

    def outside(t, q):
        rows = rows_of(q)
        mine, turned, other = PS[t, 0, rows, :], PH[0, rows, :], HT[t, rows, :]
        slant = 0.625 * (right(other) - mine) + 0.375 * (pltpu.roll(other, GRID + 1, 1) - turned)
        top = PW[0, rows, :] * (mine - other) - PW[1, rows, :] * slant
        mine, turned, other = PS[t, 1, rows, :], PH[1, rows, :], HB[t, rows, :]
        slant = 0.625 * (mine - left(other)) + 0.375 * (turned - pltpu.roll(other, GRID - 1, 1))
        bottom = PW[2, rows, :] * (mine - other) + PW[3, rows, :] * slant
        FX[0, rows, :] = top
        FX[1, rows, :] = bottom
        return top, bottom

    def add(old, new):
        return old + new

    def put(old, new):
        return new

    before_rows(0, Y, middle)
    loads[5].wait()
    for q in range(groups):
        rows = rows_of(q)
        head, foot = slice(64 * q, 64 * q + 8), slice(64 * q + 56, 64 * q + 64)
        PF[0, rows, :] = pack_first(FS[0, head, :], FS[1, head, :])
        PF[1, rows, :] = pack_last(FS[0, foot, :], FS[1, foot, :])

    arrive((cross_copy,) + section_copies(0) + row_copies(0) + (bits_copy,))
    hear(0)
    for q in range(groups // 2):
        both = BT[rows_of(q), :]
        for n, bits in enumerate((jnp.where(lo, both, half(both)), jnp.where(lo, half(both), both))):
            rows = rows_of(q + n * (groups // 2))
            k = jnp.where(has_above, KS[rows, :], zero)
            PW[0, rows, :] = jnp.where((bits & 2) != 0, k, zero) * down_scale
            PW[1, rows, :] = right(jnp.where(((bits & 4) != 0) & open_column, k, zero))

    for s in ends:
        first_apply(s, 0)
    before_rows(0, Y, outer)
    for q in range(groups):
        rows = rows_of(q)
        top, bottom = packed(DG, q)
        PI[0, rows, :] = 1.0 / (top + (PW[0, rows, :] + 0.625 * PW[1, rows, :]))
        PI[1, rows, :] = 1.0 / (bottom + (PW[2, rows, :] + 0.625 * PW[3, rows, :]))
    for q in range(groups):
        rows = rows_of(q)
        for n, part in enumerate(outside(0, q)):
            res = PF[n, rows, :] - (PY[n, rows, :] + part)
            PF[n, rows, :] = res
            PS[1, n, rows, :] = res * PI[n, rows, :]
    start(row_copies(1))
    say(1)
    for q in range(groups):
        rows = rows_of(q)
        change_rows(Y, q, FX[0, rows, :], FX[1, rows, :], add)
        change_rows(INV, q, PI[0, rows, :], PI[1, rows, :], put)

    def residual(s, total):
        for c in range(2):
            res = FS[c, raw(s), :] - Y[c, tile(s), :]
            pre = res * INV[c, tile(s), :]
            R[c, tile(s), :] = res
            Z[c, tile(s + PRED), :] = pre
            total = total + res * pre
        return total

    sum0 = zero
    for s in ends:
        sum0 = residual(s, sum0)
    start(section_copies(1))
    sum0 = over_inner(residual, sum0, 10)

    def second_apply(s, carry):
        apply(Z, W, s)
        return carry

    over_inner(second_apply, 0, APPLY_UNROLL)
    before_rows(1, W, middle)

    arrive(section_copies(1) + row_copies(1))
    hear(1)
    for s in ends:
        second_apply(s, 0)
    before_rows(1, W, outer)
    for q in range(groups):
        rows = rows_of(q)
        for n, part in enumerate(outside(1, q)):
            PS[2, n, rows, :] = (PF[n, rows, :] - (PY[n, rows, :] + part)) * PI[n, rows, :]
    start(row_copies(2))
    say(2)
    for q in range(groups):
        change_rows(W, q, FX[0, rows_of(q), :], FX[1, rows_of(q), :], add)

    def second(s, totals):
        sum1, sum2 = totals
        for c in range(2):
            gap = R[c, tile(s), :] - W[c, tile(s), :]
            u = gap * INV[c, tile(s), :]
            U[c, tile(s + PRED), :] = u
            sum1 = sum1 + gap * Z[c, tile(s + PRED), :]
            sum2 = sum2 + gap * u
        return sum1, sum2

    sums = (zero, zero)
    for s in ends:
        sums = second(s, sums)
    start(section_copies(2))
    sum1, sum2 = over_inner(second, sums, 10)
    sum3 = over_inner(lambda s, total: total + apply(U, V, s), zero, APPLY_UNROLL)
    for q in range(groups):
        for n in range(2):
            PH[n, rows_of(q), :] = half(PS[2, n, rows_of(q), :])

    arrive(section_copies(2) + row_copies(2))
    hear(2)
    for s in ends:
        sum3 = sum3 + apply(U, V, s)
    for q in range(groups):
        top, bottom = outside(2, q)
        sum3 = sum3 + (top * PS[2, 0, rows_of(q), :] + bottom * PS[2, 1, rows_of(q), :])

    row = zero
    for n, part in enumerate((sum0, sum1, sum2, sum3)):
        part = part + half(part)
        part = part + pltpu.roll(part, 32, 1)
        row = jnp.where(lane // 32 == n, part, row)
    row = jnp.sum(row, axis=0, keepdims=True)
    pending = []

    def finish_rows():
        for q in range(groups):
            change_rows(V, q, FX[0, rows_of(q), :], FX[1, rows_of(q), :], add)

    for t, group in enumerate(stages):
        totals_out[t][0] = row
        for n, offset in enumerate(group):
            copy = pltpu.make_async_remote_copy(
                src_ref=totals_out[t].at[0], dst_ref=totals_in[t].at[n],
                send_sem=tsend_sem.at[t], recv_sem=trecv_sem.at[t],
                device_id=member(offset), device_id_type=MESH,
            )
            copy.start()
        everyone = pltpu.make_async_remote_copy(
            src_ref=totals_in[t], dst_ref=totals_in[t], send_sem=tsend_sem.at[t], recv_sem=trecv_sem.at[t],
            device_id=member(group[0]), device_id_type=MESH,
        )
        if t == 0:
            finish_rows()
        everyone.wait_recv()
        pending.append(everyone)
        count = len(group)
        cuts = [count * n // 6 for n in range(7)] if count > 30 else [0, count]
        parts = [jnp.sum(totals_in[t][a:b], axis=0) for a, b in zip(cuts, cuts[1:])]
        while len(parts) > 1:
            parts = [sum(parts[n : n + 2][1:], parts[n]) for n in range(0, len(parts), 2)]
        row = row + parts[0]

    lanes = lax.broadcasted_iota(jnp.int32, (1, LANES), 1) // 32
    zz, zy, yy, ay = [jnp.sum(jnp.where(lanes == n, row, 0.0), axis=1, keepdims=True) for n in range(4)]
    curve = zz - zy
    alpha0 = zz / curve
    turn = -zy / curve
    inner1 = alpha0 * alpha0 * (yy - zy * zy / zz)
    growth = inner1 / zz
    bend = turn * turn * curve + 2.0 * turn * alpha0 * (zy - yy) + alpha0 * alpha0 * ay
    alpha1 = inner1 / (bend - growth * inner1 / alpha0)
    along = jnp.broadcast_to(alpha0 + alpha1 * (turn + growth), (8, LANES))
    across = jnp.broadcast_to(alpha1 * alpha0, (8, LANES))

    factors[0] = along
    factors[1] = across

    for t in range(3):
        sent(row_copies(t) + section_copies(t))
    sent((bits_copy, cross_copy))
    for copy in pending:
        copy.wait_send()


def finish(X, Z, U, R, W, V, factors, solved, left_over, XO, RO, sem):
    groups = XO.shape[1] // 64
    along, across = factors[0], factors[1]
    copies = []
    for part in range(PARTS):
        first, last = groups * part // PARTS, groups * (part + 1) // PARTS
        for n, (out, to) in enumerate(((XO, solved), (RO, left_over))):

            def group(q, carry):
                for i in range(8):
                    for c in range(2):
                        here = pl.ds(pl.multiple_of(64 * q + 8 * i, 8), 8)
                        held = pl.ds(pl.multiple_of(64 * q + 8 * (i + PRED), 8), 8)
                        if n == 0:
                            value = X[c, held, :] + (along * Z[c, held, :] + across * U[c, held, :])
                        else:
                            value = R[c, here, :] - (along * W[c, here, :] + across * V[c, here, :])
                        out[c, pl.ds(64 * q + i, 8, stride=8), :] = value
                return carry

            lax.fori_loop(first, last, group, 0)
            rows = pl.ds(64 * first, 64 * (last - first))
            copy = pltpu.make_async_copy(out.at[:, rows], to.at[:, rows], sem.at[2 * part + n])
            copy.start()
            copies.append(copy)
    for copy in copies:
        copy.wait()


def tiles(shard):
    *lead, sections, nodes = shard.shape
    split = shard.reshape(*lead, sections // 8, 8, nodes // LANES, LANES)
    return jnp.swapaxes(split, -3, -2).reshape(*lead, sections * nodes // LANES, LANES)


def untiled(rows, sections, nodes):
    lead = rows.shape[:-2]
    split = rows.reshape(*lead, sections // 8, nodes // LANES, 8, LANES)
    return jnp.swapaxes(split, -3, -2).reshape(*lead, sections, nodes)


def per_device(n_gz, n_rows, forces, start, spring_bits, plane_stiffness, cross_weight, anchors):
    _, sections, nodes = forces.shape
    stages = stage_groups(n_gz, n_rows)
    f32 = functools.partial(pltpu.VMEM, dtype=jnp.float32)
    own, held = 8 * sections, 8 * (sections + 2 * PRED)
    scratch = [
        pltpu.SMEM((sections,), jnp.float32),
        pltpu.SMEM((PRED, sections), jnp.float32),
        pltpu.SMEM(anchors.shape, jnp.int32),
        f32((2, own, LANES)),
        f32((2, own, LANES)),
        pltpu.VMEM((own, LANES), jnp.int32),
        *[f32((2, own, LANES)) for _ in range(2)],
        f32((3, own, LANES)),
        f32((6, own, LANES)),
        f32((PRED, own + 8 * PRED, LANES)),
        f32((sections, LANES)),
        f32((sections, LANES)),
        f32((3, 2, sections, LANES)),
        f32((3, sections, LANES)),
        f32((3, sections, LANES)),
        pltpu.VMEM((sections // 2, LANES), jnp.int32),
        pltpu.VMEM((sections // 2, LANES), jnp.int32),
        f32((4, sections, LANES)),
        *[f32((2, sections, LANES)) for _ in range(5)],
        *[f32((1, 1, LANES)) for _ in stages],
        *[f32((len(group), 1, LANES)) for group in stages],
        pltpu.SemaphoreType.DMA((6,)),
        pltpu.SemaphoreType.DMA((14,)),
        pltpu.SemaphoreType.DMA((14,)),
        pltpu.SemaphoreType.DMA((len(stages),)),
        pltpu.SemaphoreType.DMA((len(stages),)),
        pltpu.SemaphoreType.REGULAR((3,)),
    ]
    kept = [(2, held, LANES)] * 3 + [(2, own, LANES)] * 3 + [(2, 8, LANES)]
    arguments = (tiles(forces), tiles(start), tiles(spring_bits), plane_stiffness, cross_weight, anchors)
    parts = pl.pallas_call(
        functools.partial(kernel, n_gz, n_rows, anchors.shape[0], stages),
        out_shape=[pltpu.VMEM(shape, jnp.float32) for shape in kept],
        in_specs=[pl.BlockSpec(memory_space=pltpu.HBM)] * 6,
        out_specs=[pl.BlockSpec(memory_space=pltpu.VMEM)] * 7,
        scratch_shapes=scratch,
        compiler_params=pltpu.CompilerParams(
            collective_id=0, has_side_effects=True, vmem_limit_bytes=24 * 1024 * 1024
        ),
        name="cg",
    )(*[pltpu.with_memory_space_constraint(a, pltpu.HBM) for a in arguments])
    shape = jax.ShapeDtypeStruct((2, own, LANES), jnp.float32)
    solved, left_over = pl.pallas_call(
        finish,
        out_shape=(shape, shape),
        in_specs=[pl.BlockSpec(memory_space=pltpu.VMEM)] * 7,
        out_specs=[pl.BlockSpec(memory_space=pltpu.HBM)] * 2,
        scratch_shapes=[f32((2, own, LANES)), f32((2, own, LANES)), pltpu.SemaphoreType.DMA((2 * PARTS,))],
        compiler_params=pltpu.CompilerParams(vmem_limit_bytes=8 * 1024 * 1024),
        name="finish",
    )(*parts)
    return untiled(solved, sections, nodes), untiled(left_over, sections, nodes)


def solution(mesh):
    return jax.shard_map(
        functools.partial(per_device, mesh.shape["gz"], mesh.shape["rows"]),
        mesh=mesh,
        in_specs=(P(None, "gz", "rows"), P(None, "gz", "rows"), P("gz", "rows"), P("gz"), P(None, "gz"), P()),
        out_specs=(P(None, "gz", "rows"), P(None, "gz", "rows")),
        check_vma=False,
    )
```

```python
import functools

import jax
import jax.numpy as jnp
from jax import lax
from jax.experimental import pallas as pl
from jax.experimental.pallas import tpu as pltpu
from jax.sharding import PartitionSpec as P

GRID = 64
PRED = 3
LANES = 128
PARTS = 6
APPLY_UNROLL = 18
MESH = pl.DeviceIdType.MESH

damping = 0.05
anchor_stiffness = 20.0


def digit_sizes(size):
    return (4, 8, 2) if size == 64 else (1, size // 2, 2)


def stage_groups(size, rows):
    ny, nz, nc = digit_sizes(size)
    twin = [(0, 0, c, 0) for c in range(1, nc)]
    rest = [(y, z, 0, x) for y in range(ny) for z in range(nz) for x in range(rows)][1:]

    def hops(offset):
        return sum(min(d, n - d) for d, n in zip(offset, (ny, nz, nc, rows)))

    return [sorted(group, key=hops, reverse=True) for group in (twin, rest) if group]


def kernel(
    n_gz, n_rows, n_anchors, stages,
    f_hbm, x_hbm, b_hbm, xtile_hbm, btile_hbm, stiff_hbm, cross_hbm, anchors_hbm,
    X, Z, U, R, W, V, factors,
    stiff, cross, anchors,
    XS, FS, BS, XE, BE, Y, INV, DG, WP, K, TE, KS,
    PS, HT, HB, BO, BT, PW, PI, PY, PH, PF, FX, FH, QS, HQ, HI, *rest,
):
    n_stages = len(stages)
    totals_out, totals_in = rest[:n_stages], rest[n_stages : 2 * n_stages]
    load_sem, send_sem, recv_sem, tsend_sem, trecv_sem, word_sem = rest[2 * n_stages :]
    sections = TE.shape[0]
    groups = sections // 8
    g, r = lax.axis_index("gz"), lax.axis_index("rows")
    has_prev, has_next, has_above, has_below = g > 0, g < n_gz - 1, r > 0, r < n_rows - 1
    prev, nxt = {"gz": g - 1, "rows": r}, {"gz": g + 1, "rows": r}
    above, below = {"gz": g, "rows": r - 1}, {"gz": g, "rows": r + 1}

    barrier = pltpu.get_barrier_semaphore()

    def signal(sem, links):
        for here, device in links:
            pl.when(here)(functools.partial(pl.semaphore_signal, sem, 1, device_id=device, device_id_type=MESH))

    def count(links):
        return sum(jnp.where(here, 1, 0) for here, _ in links)

    beside = ((has_prev, prev), (has_next, nxt))
    signal(barrier, beside)
    own = 8 * sections
    head, body, foot = pl.ds(0, 64), pl.ds(64, own - 128), pl.ds(own - 64, 64)
    loads = [
        pltpu.make_async_copy(src, dst, load_sem.at[i])
        for i, (src, dst) in enumerate(
            [
                (stiff_hbm, stiff),
                (cross_hbm, cross),
                (b_hbm.at[head], BS.at[head]),
                (btile_hbm.at[:, 7], BE),
                (xtile_hbm.at[:, :, 0], XE.at[0]),
                (xtile_hbm.at[:, :, 7], XE.at[1]),
                (x_hbm.at[:, head], XS.at[:, head]),
                (x_hbm.at[:, foot], XS.at[:, foot]),
                (anchors_hbm, anchors),
                (b_hbm.at[foot], BS.at[foot]),
            ]
            + ([(b_hbm.at[body], BS.at[body]), (x_hbm.at[:, body], XS.at[:, body])] if sections > 16 else [])
            + [(f_hbm, FS)]
        )
    ]
    for load in loads[:-1]:
        load.start()
    ny, nz, nc = digit_sizes(n_gz)
    my_digits = (g // (nz * nc), (g // nc) & (nz - 1), g & (nc - 1), r)

    def member(offset):
        y, z, c, x = [(d + o) & (n - 1) for d, o, n in zip(my_digits, offset, (ny, nz, nc, n_rows))]
        return {"gz": (y * nz + z) * nc + c, "rows": x}

    def along_lines(by, axes="xyz"):
        links = []
        for axis, size, at in (("x", n_rows, r), ("y", ny, my_digits[0]), ("z", nz, my_digits[1])):
            step = {"x": 0, "y": nz * nc, "z": nc}[axis] * by
            if size > by and axis in axes:
                move = by if axis == "x" else 0
                links.append((at >= by, {"gz": g - step, "rows": r - move}))
                links.append((at < size - by, {"gz": g + step, "rows": r + move}))
        return links

    lines = along_lines(1)
    signal(barrier, lines)
    word = (
        lines,
        along_lines(2),
        along_lines(4, "z"),
        [(None, member((0, 0, 0, x))) for x in range(1, n_rows)],
        [(None, member((y, 0, 0, 0))) for y in range(1, ny)],
    )

    def say(t):
        for here, device in word[t]:
            tell = functools.partial(pl.semaphore_signal, word_sem.at[t], 1, device_id=device, device_id_type=MESH)
            tell() if here is None else pl.when(here)(tell)

    def hear(t):
        if word[t]:
            told = len(word[t]) if word[t][0][0] is None else count(word[t])
            pl.semaphore_wait(word_sem.at[t], told)

    lane = lax.broadcasted_iota(jnp.int32, (8, LANES), 1)
    sub = lax.broadcasted_iota(jnp.int32, (8, LANES), 0)
    lo = lane < GRID
    column = lane % GRID
    open_column = column < GRID - 1
    inner_row = (2 * sub + lane // GRID) < 15
    mask_right = jnp.where(open_column, 1, 0)
    mask_down = jnp.where(inner_row, 2, 0)
    mask_diag = jnp.where(open_column & inner_row, 4, 0)
    down_scale = jnp.where(lo, 0.25, 1.0).astype(jnp.float32)
    zero = jnp.zeros((8, LANES), jnp.float32)

    def half(v):
        return pltpu.roll(v, GRID, 1)

    def left(v):
        return pltpu.roll(v, LANES - 1, 1)

    def right(v):
        return pltpu.roll(v, 1, 1)

    def lowered(v, by):
        return pltpu.roll(jnp.where(lo, v, pltpu.roll(v, 1, 0)), by, 1)

    def tile(s):
        return pl.ds(pl.multiple_of(8 * s, 8), 8)

    def raw(s):
        return pl.ds((s // 8) * 64 + s % 8, 8, stride=8)

    def pack_last(a, b):
        return jnp.where(lo, half(a), b)

    def pack_first(a, b):
        return jnp.where(lo, a, half(b))

    base = g * sections

    def cross_weights(s, bits):
        for j in range(PRED):
            kj = jnp.where(base + s > j, cross[j, s], 0.0) if isinstance(s, int) and s < PRED else cross[j, s]
            K[j, tile(s), :] = jnp.where((bits & (8 << j)) != 0, jnp.full((8, LANES), kj, jnp.float32), zero)

    def plane_weights(s, bits):
        KS[pl.ds(s, 1), :] = jnp.full((1, LANES), stiff[s], jnp.float32)
        k = jnp.full((8, LANES), stiff[s], jnp.float32)
        wr = jnp.where((bits & mask_right) != 0, k, zero)
        wd = jnp.where((bits & mask_down) != 0, k, zero)
        wg = jnp.where((bits & mask_diag) != 0, k, zero)
        for n, w in enumerate((wr, right(wr), wd, lowered(wd, GRID), wg, lowered(wg, GRID + 1))):
            WP[n, tile(s), :] = w

    for load in loads[:8]:
        load.wait()
    for s in range(PRED):
        cross_weights(s, BS[raw(s), :])

    for q in range(groups // 2):
        BO[8 * q : 8 * q + 8, :] = jnp.where(lo, half(BE[q]), BE[q + groups // 2])

    for c in range(2):
        for s in list(range(PRED)) + list(range(sections - PRED, sections)):
            X[c, 8 * (s + PRED) : 8 * (s + PRED) + 8, :] = XS[c, pl.ds((s // 8) * 64 + s % 8, 8, stride=8), :]
    for q in range(groups):
        rows = slice(8 * q, 8 * q + 8)
        PS[0, 0, rows, :] = pack_first(XE[0, 0, q], XE[0, 1, q])
        PS[0, 1, rows, :] = pack_last(XE[1, 0, q], XE[1, 1, q])

    pl.semaphore_wait(barrier, count(beside) + count(lines))

    def remote(src, dst, at, device):
        return pltpu.make_async_remote_copy(
            src_ref=src, dst_ref=dst, send_sem=send_sem.at[at], recv_sem=recv_sem.at[at],
            device_id=device, device_id_type=MESH,
        )

    edge = 8 * PRED

    def row_copies(t):
        return (
            (has_below, has_above, remote(PS.at[t, 1], HT.at[t], 4 * t, below)),
            (has_above, has_below, remote(PS.at[t, 0], HB.at[t], 4 * t + 1, above)),
        )

    def section_copies(t):
        v = (X, Z, U)[t]
        return (
            (has_next, has_prev, remote(v.at[:, pl.ds(own, edge)], v.at[:, pl.ds(0, edge)], 4 * t + 2, nxt)),
            (has_prev, has_next, remote(v.at[:, pl.ds(edge, edge)], v.at[:, pl.ds(own + edge, edge)], 4 * t + 3, prev)),
        )

    def both_ways(part, src, to, at):
        return (
            (has_below, has_above, remote(src.at[1, part], to.at[0, part], at, below)),
            (has_above, has_below, remote(src.at[0, part], to.at[1, part], at + 1, above)),
        )

    inverse_copies = both_ways(pl.ds(0, sections), PI, HI, 14)
    middle_copies = both_ways(pl.ds(8, sections - 16), QS, HQ, 8) if sections > 16 else ()
    outer_copies = both_ways(pl.ds(0, 8), QS, HQ, 16) + both_ways(pl.ds(sections - 8, 8), QS, HQ, 18)

    bits_copy = (has_below, has_above, remote(BO, BT, 12, below))
    cross_copy = (has_prev, has_next, remote(K.at[:, pl.ds(0, edge)], K.at[:, pl.ds(own, edge)], 13, prev))

    def start(copies):
        for sends, _, copy in copies:
            pl.when(sends)(copy.start)

    def arrive(copies):
        for _, receives, copy in copies:
            pl.when(receives)(copy.wait_recv)

    def sent(copies):
        for sends, _, copy in copies:
            pl.when(sends)(copy.wait_send)

    start(row_copies(0) + section_copies(0) + (cross_copy, bits_copy))
    loads[-1].start()
    say(0)

    for load in loads[8:-1]:
        load.wait()

    def anchor_step(i, hits):
        for n in range(8):
            a = anchors[8 * i + n] - base
            hits = tuple(jnp.where(sub == a - 8 * q, 1, hit) for q, hit in enumerate(hits))
        return hits

    hits = lax.fori_loop(0, n_anchors // 8, anchor_step, tuple(jnp.zeros((8, LANES), jnp.int32) for _ in range(groups)))
    for q in range(groups):
        TE[8 * q : 8 * q + 8, :] = jnp.where(hits[q] > 0, damping + anchor_stiffness, damping).astype(jnp.float32)

    wide = jnp.zeros((2, edge, LANES), jnp.float32)

    @pl.when(jnp.logical_not(has_prev))
    def _():
        for v in (X, Z, U):
            v[:, 0:edge, :] = wide

    @pl.when(jnp.logical_not(has_next))
    def _():
        for v in (X, Z, U):
            v[:, own + edge : own + 2 * edge, :] = wide
        K[:, own : own + edge, :] = jnp.zeros((PRED, edge, LANES), jnp.float32)

    @pl.when(jnp.logical_not(has_above))
    def _():
        HT[...] = jnp.zeros(HT.shape, jnp.float32)
        HI[0] = jnp.zeros(HI.shape[1:], jnp.float32)
        HQ[0] = jnp.zeros(HQ.shape[1:], jnp.float32)
        BT[...] = jnp.zeros(BT.shape, jnp.int32)

    @pl.when(jnp.logical_not(has_below))
    def _():
        HB[...] = jnp.zeros(HB.shape, jnp.float32)
        HI[1] = jnp.zeros(HI.shape[1:], jnp.float32)
        HQ[1] = jnp.zeros(HQ.shape[1:], jnp.float32)

    ends = list(range(PRED)) + list(range(sections - PRED, sections))
    inner = sections - 2 * PRED

    def over_inner(body, carry, most):
        unroll = next(n for n in range(most, 0, -1) if inner % n == 0)

        def step(i, carry):
            for n in range(unroll):
                carry = body(PRED + unroll * i + n, carry)
            return carry

        return lax.fori_loop(0, inner // unroll, step, carry)

    def fill(q, carry):
        for i in range(8):
            s = 8 * q + i
            bits = BS[pl.ds(64 * q + i, 8, stride=8), :]
            plane_weights(s, bits)
            if not isinstance(s, int) or s >= PRED:
                cross_weights(s, bits)
            if not isinstance(s, int) or s not in ends:
                for c in range(2):
                    X[c, tile(s + PRED), :] = XS[c, pl.ds(64 * q + i, 8, stride=8), :]
        return carry

    def fill_pair(p, carry):
        return fill(2 * p + 2, fill(2 * p + 1, carry))

    lax.fori_loop(0, (groups - 2) // 2, fill_pair, 0)
    fill(0, 0)
    fill(groups - 1, 0)

    def apply(v, out, s, first=False):
        wr, wl, wd, wu, wg, wv = [WP[n, tile(s), :] for n in range(6)]
        back = [K[j, tile(s), :] for j in range(PRED)]
        ahead = [K[j, tile(s + j + 1), :] for j in range(PRED)]
        if first:
            tether = jnp.broadcast_to(TE[pl.ds(s, 1), :], (8, LANES))
            shared = tether + ((back[0] + ahead[0]) + (back[1] + ahead[1]) + (back[2] + ahead[2]))
            shared = shared + 0.625 * (wg + wv)
            across, along = wr + wl, wd + wu
            own_weight = [shared + across + 0.25 * along, shared + 0.25 * across + along]
            mixed = 0.375 * (wg + wv)
            DG[2, tile(s), :] = mixed
            for c in range(2):
                DG[c, tile(s), :] = own_weight[c]
                INV[c, tile(s), :] = 1.0 / own_weight[c]
        else:
            own_weight, mixed = [DG[c, tile(s), :] for c in range(2)], DG[2, tile(s), :]
        mine = [v[c, tile(s + PRED), :] for c in range(2)]
        sides, lines, slants = [], [], []
        for c in range(2):
            after = jnp.where(lo, v[c, pl.ds(8 * (s + PRED) + 1, 8), :], mine[c])
            before = jnp.where(lo, mine[c], v[c, pl.ds(8 * (s + PRED) - 1, 8), :])
            sides.append(wr * left(mine[c]) + wl * right(mine[c]))
            lines.append(wd * half(after) + wu * half(before))
            slants.append(wg * pltpu.roll(after, GRID - 1, 1) + wv * pltpu.roll(before, GRID + 1, 1))
        pulls = [
            (sides[0] + 0.25 * lines[0]) + (0.625 * slants[0] + 0.375 * slants[1]),
            (0.25 * sides[1] + lines[1]) + (0.375 * slants[0] + 0.625 * slants[1]),
        ]
        done = []
        for c in range(2):
            ties = [
                back[j] * v[c, tile(s + PRED - j - 1), :] + ahead[j] * v[c, tile(s + PRED + j + 1), :]
                for j in range(PRED)
            ]
            total = (own_weight[c] * mine[c] + mixed * mine[1 - c]) - (pulls[c] + (ties[0] + ties[1] + ties[2]))
            out[c, tile(s), :] = total
            done.append(total)
        return mine[0] * done[0] + mine[1] * done[1]

    def first_apply(s, carry):
        apply(X, Y, s, first=True)
        return carry

    over_inner(first_apply, 0, APPLY_UNROLL)

    def rows_of(q):
        return slice(8 * q, 8 * q + 8)

    def packed(ref, q):
        at = [[ref[c, pl.ds(64 * q + line, 8, stride=8), :] for c in range(2)] for line in (0, 7)]
        return pack_first(*at[0]), pack_last(*at[1])

    def spread(top, bottom):
        return (top, half(top)), (half(bottom), bottom)

    def change_rows(ref, q, top, bottom, change):
        for line, keep_lo, parts in zip((0, 7), (False, True), spread(top, bottom)):
            for c in range(2):
                to = pl.ds(64 * q + line, 8, stride=8)
                old = ref[c, to, :]
                new = change(old, parts[c])
                ref[c, to, :] = jnp.where(lo, old, new) if keep_lo else jnp.where(lo, new, old)

    for q in range(groups):
        rows = rows_of(q)
        bits = BE[q]
        bits = jnp.where(lo, half(bits), bits)
        k = jnp.where(has_below, KS[rows, :], zero)
        PW[2, rows, :] = jnp.where((bits & 2) != 0, k, zero) * down_scale
        slant_weight = jnp.where(((bits & 4) != 0) & open_column, k, zero)
        PW[3, rows, :] = slant_weight
        PW[5, rows, :] = right(slant_weight)

    middle = range(1, groups - 1)
    outer = sorted({0, groups - 1})

    def before_rows(t, out, some):
        for q in some:
            rows = rows_of(q)
            for n, part in enumerate(packed(out, q)):
                PY[n, rows, :] = part
                PH[n, rows, :] = half(PS[t, n, rows, :])

    def pull_up(mine, turned, other, down, slant_shifted):
        slant = 0.625 * (right(other) - mine) + 0.375 * (pltpu.roll(other, GRID + 1, 1) - turned)
        return down * (mine - other) - slant_shifted * slant

    def pull_down(mine, turned, other, down, slant_weight):
        slant = 0.625 * (mine - left(other)) + 0.375 * (turned - pltpu.roll(other, GRID - 1, 1))
        return down * (mine - other) + slant_weight * slant

    def outside(t, q):
        rows = rows_of(q)
        top = pull_up(PS[t, 0, rows, :], PH[0, rows, :], HT[t, rows, :], PW[0, rows, :], PW[1, rows, :])
        bottom = pull_down(PS[t, 1, rows, :], PH[1, rows, :], HB[t, rows, :], PW[2, rows, :], PW[3, rows, :])
        FX[0, rows, :] = top
        FX[1, rows, :] = bottom
        return top, bottom

    def outside_there(t, q):
        rows = rows_of(q)
        above_row, below_row = HT[t, rows, :], HB[t, rows, :]
        FH[0, rows, :] = pull_down(above_row, half(above_row), PS[t, 0, rows, :], PW[0, rows, :], PW[4, rows, :])
        FH[1, rows, :] = pull_up(below_row, half(below_row), PS[t, 1, rows, :], PW[2, rows, :], PW[5, rows, :])

    def add(old, new):
        return old + new

    def put(old, new):
        return new

    before_rows(0, Y, middle)
    loads[-1].wait()
    for q in range(groups):
        rows = rows_of(q)
        head, foot = slice(64 * q, 64 * q + 8), slice(64 * q + 56, 64 * q + 64)
        PF[0, rows, :] = pack_first(FS[0, head, :], FS[1, head, :])
        PF[1, rows, :] = pack_last(FS[0, foot, :], FS[1, foot, :])

    hear(0)
    say(1)
    arrive((cross_copy,) + section_copies(0) + row_copies(0) + (bits_copy,))
    for q in range(groups // 2):
        both = BT[rows_of(q), :]
        for n, bits in enumerate((jnp.where(lo, both, half(both)), jnp.where(lo, half(both), both))):
            rows = rows_of(q + n * (groups // 2))
            k = jnp.where(has_above, KS[rows, :], zero)
            PW[0, rows, :] = jnp.where((bits & 2) != 0, k, zero) * down_scale
            slant_weight = jnp.where(((bits & 4) != 0) & open_column, k, zero)
            PW[1, rows, :] = right(slant_weight)
            PW[4, rows, :] = slant_weight

    for s in ends:
        first_apply(s, 0)
    before_rows(0, Y, outer)
    for q in range(groups):
        rows = rows_of(q)
        top, bottom = packed(DG, q)
        PI[0, rows, :] = 1.0 / (top + (PW[0, rows, :] + 0.625 * PW[1, rows, :]))
        PI[1, rows, :] = 1.0 / (bottom + (PW[2, rows, :] + 0.625 * PW[3, rows, :]))
    for q in range(groups):
        rows = rows_of(q)
        for n, part in enumerate(outside(0, q)):
            res = PF[n, rows, :] - (PY[n, rows, :] + part)
            PF[n, rows, :] = res
            PS[1, n, rows, :] = res * PI[n, rows, :]
    def residual(s, total):
        for c in range(2):
            res = FS[c, raw(s), :] - Y[c, tile(s), :]
            pre = res * INV[c, tile(s), :]
            R[c, tile(s), :] = res
            Z[c, tile(s + PRED), :] = pre
            total = total + res * pre
        return total

    def change_first(q):
        rows = rows_of(q)
        change_rows(Y, q, FX[0, rows, :], FX[1, rows, :], add)
        change_rows(INV, q, PI[0, rows, :], PI[1, rows, :], put)

    for q in outer:
        change_first(q)
    sum0 = zero
    for s in ends:
        sum0 = residual(s, sum0)
    start(row_copies(1) + section_copies(1) + inverse_copies)
    for q in middle:
        change_first(q)
    sum0 = over_inner(residual, sum0, 10)
    hear(1)
    say(2)

    def second_apply(s, carry):
        apply(Z, W, s)
        return carry

    over_inner(second_apply, 0, APPLY_UNROLL)
    before_rows(1, W, middle)

    def send_part(some):
        for q in some:
            for n in range(2):
                QS[n, rows_of(q), :] = PF[n, rows_of(q), :] - PY[n, rows_of(q), :]

    send_part(middle)
    start(middle_copies)

    arrive(section_copies(1) + row_copies(1))
    for s in ends:
        second_apply(s, 0)
    before_rows(1, W, outer)
    send_part(outer)
    start(outer_copies)
    def own_part(some):
        for q in some:
            rows = rows_of(q)
            for n, part in enumerate(outside(1, q)):
                PS[2, n, rows, :] = (QS[n, rows, :] - part) * PI[n, rows, :]

    own_part(outer)
    for q in outer:
        change_rows(W, q, FX[0, rows_of(q), :], FX[1, rows_of(q), :], add)

    def second(s, totals):
        sum1, sum2 = totals
        for c in range(2):
            gap = R[c, tile(s), :] - W[c, tile(s), :]
            u = gap * INV[c, tile(s), :]
            U[c, tile(s + PRED), :] = u
            sum1 = sum1 + gap * Z[c, tile(s + PRED), :]
            sum2 = sum2 + gap * u
        return sum1, sum2

    sums = (zero, zero)
    for s in ends:
        sums = second(s, sums)
    start(section_copies(2))
    own_part(middle)
    for q in range(groups):
        outside_there(1, q)
    for q in middle:
        change_rows(W, q, FX[0, rows_of(q), :], FX[1, rows_of(q), :], add)
    sum1, sum2 = over_inner(second, sums, 10)
    hear(2)
    say(3)
    sum3 = over_inner(lambda s, total: total + apply(U, V, s), zero, APPLY_UNROLL)
    for q in range(groups):
        for n in range(2):
            PH[n, rows_of(q), :] = half(PS[2, n, rows_of(q), :])

    hear(3)
    say(4)
    arrive(section_copies(2) + inverse_copies + middle_copies + outer_copies)
    for q in range(groups):
        rows = rows_of(q)
        HT[2, rows, :] = (HQ[0, rows, :] - FH[0, rows, :]) * HI[0, rows, :]
        HB[2, rows, :] = (HQ[1, rows, :] - FH[1, rows, :]) * HI[1, rows, :]
    for s in ends:
        sum3 = sum3 + apply(U, V, s)
    for q in range(groups):
        top, bottom = outside(2, q)
        sum3 = sum3 + (top * PS[2, 0, rows_of(q), :] + bottom * PS[2, 1, rows_of(q), :])

    row = zero
    for n, part in enumerate((sum0, sum1, sum2, sum3)):
        part = part + half(part)
        part = part + pltpu.roll(part, 32, 1)
        row = jnp.where(lane // 32 == n, part, row)
    row = jnp.sum(row, axis=0, keepdims=True)
    pending = []

    def finish_rows():
        for q in range(groups):
            change_rows(V, q, FX[0, rows_of(q), :], FX[1, rows_of(q), :], add)

    for t, group in enumerate(stages):
        if t == 1:
            hear(4)
        totals_out[t][0] = row
        for n, offset in enumerate(group):
            copy = pltpu.make_async_remote_copy(
                src_ref=totals_out[t].at[0], dst_ref=totals_in[t].at[n],
                send_sem=tsend_sem.at[t], recv_sem=trecv_sem.at[t],
                device_id=member(offset), device_id_type=MESH,
            )
            copy.start()
        everyone = pltpu.make_async_remote_copy(
            src_ref=totals_in[t], dst_ref=totals_in[t], send_sem=tsend_sem.at[t], recv_sem=trecv_sem.at[t],
            device_id=member(group[0]), device_id_type=MESH,
        )
        if t == 0:
            finish_rows()
        everyone.wait_recv()
        pending.append(everyone)
        members = len(group)
        cuts = [members * n // 6 for n in range(7)] if members > 30 else [0, members]
        parts = [jnp.sum(totals_in[t][a:b], axis=0) for a, b in zip(cuts, cuts[1:])]
        while len(parts) > 1:
            parts = [sum(parts[n : n + 2][1:], parts[n]) for n in range(0, len(parts), 2)]
        row = row + parts[0]

    lanes = lax.broadcasted_iota(jnp.int32, (1, LANES), 1) // 32
    zz, zy, yy, ay = [jnp.sum(jnp.where(lanes == n, row, 0.0), axis=1, keepdims=True) for n in range(4)]
    curve = zz - zy
    alpha0 = zz / curve
    turn = -zy / curve
    inner1 = alpha0 * alpha0 * (yy - zy * zy / zz)
    growth = inner1 / zz
    bend = turn * turn * curve + 2.0 * turn * alpha0 * (zy - yy) + alpha0 * alpha0 * ay
    alpha1 = inner1 / (bend - growth * inner1 / alpha0)
    along = jnp.broadcast_to(alpha0 + alpha1 * (turn + growth), (8, LANES))
    across = jnp.broadcast_to(alpha1 * alpha0, (8, LANES))

    factors[0] = along
    factors[1] = across

    for t in range(3):
        sent((row_copies(t) if t < 2 else ()) + section_copies(t))
    sent((bits_copy, cross_copy) + inverse_copies + middle_copies + outer_copies)
    for copy in pending:
        copy.wait_send()


def finish(X, Z, U, R, W, V, factors, solved, left_over, XO, RO, sem):
    groups = XO.shape[1] // 64
    along, across = factors[0], factors[1]
    copies = []
    count = min(PARTS, groups)
    for part in range(count):
        first, last = groups * part // count, groups * (part + 1) // count
        for n, (out, to) in enumerate(((XO, solved), (RO, left_over))):

            def group(q, carry):
                for i in range(8):
                    for c in range(2):
                        here = pl.ds(pl.multiple_of(64 * q + 8 * i, 8), 8)
                        held = pl.ds(pl.multiple_of(64 * q + 8 * (i + PRED), 8), 8)
                        if n == 0:
                            value = X[c, held, :] + (along * Z[c, held, :] + across * U[c, held, :])
                        else:
                            value = R[c, here, :] - (along * W[c, here, :] + across * V[c, here, :])
                        out[c, pl.ds(64 * q + i, 8, stride=8), :] = value
                return carry

            lax.fori_loop(first, last, group, 0)
            rows = pl.ds(64 * first, 64 * (last - first))
            copy = pltpu.make_async_copy(out.at[:, rows], to.at[:, rows], sem.at[2 * part + n])
            copy.start()
            copies.append(copy)
    for copy in copies:
        copy.wait()


def tiles(shard):
    *lead, sections, nodes = shard.shape
    split = shard.reshape(*lead, sections // 8, 8, nodes // LANES, LANES)
    return jnp.swapaxes(split, -3, -2).reshape(*lead, sections * nodes // LANES, LANES)


def untiled(rows, sections, nodes):
    lead = rows.shape[:-2]
    split = rows.reshape(*lead, sections // 8, nodes // LANES, 8, LANES)
    return jnp.swapaxes(split, -3, -2).reshape(*lead, sections, nodes)


def per_device(n_gz, n_rows, forces, start, spring_bits, plane_stiffness, cross_weight, anchors):
    _, sections, nodes = forces.shape
    stages = stage_groups(n_gz, n_rows)
    f32 = functools.partial(pltpu.VMEM, dtype=jnp.float32)
    own, held = 8 * sections, 8 * (sections + 2 * PRED)
    scratch = [
        pltpu.SMEM((sections,), jnp.float32),
        pltpu.SMEM((PRED, sections), jnp.float32),
        pltpu.SMEM(anchors.shape, jnp.int32),
        f32((2, own, LANES)),
        f32((2, own, LANES)),
        pltpu.VMEM((own, LANES), jnp.int32),
        f32((2, 2, sections // 8, 8, LANES)),
        pltpu.VMEM((sections // 8, 8, LANES), jnp.int32),
        *[f32((2, own, LANES)) for _ in range(2)],
        f32((3, own, LANES)),
        f32((6, own, LANES)),
        f32((PRED, own + 8 * PRED, LANES)),
        f32((sections, LANES)),
        f32((sections, LANES)),
        f32((3, 2, sections, LANES)),
        f32((3, sections, LANES)),
        f32((3, sections, LANES)),
        pltpu.VMEM((sections // 2, LANES), jnp.int32),
        pltpu.VMEM((sections // 2, LANES), jnp.int32),
        f32((6, sections, LANES)),
        *[f32((2, sections, LANES)) for _ in range(9)],
        *[f32((1, 1, LANES)) for _ in stages],
        *[f32((len(group), 1, LANES)) for group in stages],
        pltpu.SemaphoreType.DMA((13,)),
        pltpu.SemaphoreType.DMA((20,)),
        pltpu.SemaphoreType.DMA((20,)),
        pltpu.SemaphoreType.DMA((len(stages),)),
        pltpu.SemaphoreType.DMA((len(stages),)),
        pltpu.SemaphoreType.REGULAR((5,)),
    ]
    kept = [(2, held, LANES)] * 3 + [(2, own, LANES)] * 3 + [(2, 8, LANES)]
    shaped = tiles(start), tiles(spring_bits)
    split = [a.reshape(*a.shape[:-2], sections // 8, 8, 8, LANES) for a in shaped]
    arguments = (tiles(forces), *shaped, *split, plane_stiffness, cross_weight, anchors)
    parts = pl.pallas_call(
        functools.partial(kernel, n_gz, n_rows, anchors.shape[0], stages),
        out_shape=[pltpu.VMEM(shape, jnp.float32) for shape in kept],
        in_specs=[pl.BlockSpec(memory_space=pltpu.HBM)] * 8,
        out_specs=[pl.BlockSpec(memory_space=pltpu.VMEM)] * 7,
        scratch_shapes=scratch,
        compiler_params=pltpu.CompilerParams(
            collective_id=0, has_side_effects=True, vmem_limit_bytes=24 * 1024 * 1024
        ),
        name="cg",
    )(*[pltpu.with_memory_space_constraint(a, pltpu.HBM) for a in arguments])
    shape = jax.ShapeDtypeStruct((2, own, LANES), jnp.float32)
    solved, left_over = pl.pallas_call(
        finish,
        out_shape=(shape, shape),
        in_specs=[pl.BlockSpec(memory_space=pltpu.VMEM)] * 7,
        out_specs=[pl.BlockSpec(memory_space=pltpu.HBM)] * 2,
        scratch_shapes=[f32((2, own, LANES)), f32((2, own, LANES)), pltpu.SemaphoreType.DMA((2 * PARTS,))],
        compiler_params=pltpu.CompilerParams(vmem_limit_bytes=8 * 1024 * 1024),
        name="finish",
    )(*parts)
    return untiled(solved, sections, nodes), untiled(left_over, sections, nodes)


def solution(mesh):
    return jax.shard_map(
        functools.partial(per_device, mesh.shape["gz"], mesh.shape["rows"]),
        mesh=mesh,
        in_specs=(P(None, "gz", "rows"), P(None, "gz", "rows"), P("gz", "rows"), P("gz"), P(None, "gz"), P()),
        out_specs=(P(None, "gz", "rows"), P(None, "gz", "rows")),
        check_vma=False,
    )
```
